512 devices in a mesh: row: 32 (over z, x_lo, core), col: 16 (over y, x_hi).
Axes of the slice: x: 4 (x_hi: 2, x_lo: 2; x = x_hi * 2 + x_lo), y: 8, z: 8, core: 2. Of those that a mesh axis runs over, the one named last changes fastest.
Arguments:
- substrate: float32 [4096, 4096], P('row', 'col'), may hold values from 0.05 to 0.95
- activator: float32 [4096, 4096], P('row', 'col'), may hold values from 0 to 0.45
Outputs:
- substrate_section: float32 [4096, 4096], P('row', 'col')
- activator_section: float32 [4096, 4096], P('row', 'col')
The draws below stay inside these ranges and needn't reach their ends.
All inputs are finite; a program needn't handle non-finite values.
Results may differ from the reference program's by a relative error of at most 0.00023.
Values sent between devices are 32-bit elements; how exact they have to be, the bound alone decides.
No kernel may reach another device: no remote copies, remote signals or barrier semaphores. Data moves between devices by JAX's collectives and lax.ppermute only.
A program may use at most 64 MiB of HBM per device.

```python
import math
import jax
import jax.numpy as jnp

NX = 4096
NY = 4096


def smooth_part(key):
    orders = jnp.arange(1, 5, dtype=jnp.float32)
    row_coords = jnp.arange(NX, dtype=jnp.float32) / NX
    col_coords = jnp.arange(NY, dtype=jnp.float32) / NY
    row_angles = 2.0 * math.pi * orders[:, None] * row_coords[None, :]
    col_angles = 2.0 * math.pi * orders[:, None] * col_coords[None, :]
    basis_rows = jnp.concatenate([jnp.cos(row_angles), jnp.sin(row_angles)], axis=0)
    basis_cols = jnp.concatenate([jnp.cos(col_angles), jnp.sin(col_angles)], axis=0)
    coefficients = jax.random.normal(key, (8, 8), jnp.float32)
    mixed = jnp.dot(coefficients, basis_cols, preferred_element_type=jnp.float32)
    return jnp.dot(basis_rows.T, mixed, preferred_element_type=jnp.float32) / 4.0


def draw_substrate(key, part):
    smooth = smooth_part(jax.random.fold_in(key, 11))
    rough_key = jax.random.fold_in(key, 12)
    rough_part = jax.random.uniform(rough_key, (NX, NY), jnp.float32, -1.0, 1.0)
    return (0.55 + 0.2 * jnp.tanh(smooth) + 0.15 * rough_part).astype(jnp.float32)


def draw_activator(key, part):
    smooth = smooth_part(jax.random.fold_in(key, 23))
    rough_key = jax.random.fold_in(key, 24)
    rough_part = jax.random.uniform(rough_key, (NX, NY), jnp.float32, -1.0, 1.0)
    return (0.25 + 0.08 * jnp.tanh(smooth) + 0.08 * rough_part).astype(jnp.float32)


def setup_inputs(seed: int = 0) -> dict:
    key_of = jax.random.split(jax.random.key(seed), 3)
    substrate = draw_substrate(jax.random.fold_in(key_of[2], 71), 0)
    activator = draw_activator(jax.random.fold_in(key_of[2], 71), 0)
    return dict(substrate=substrate, activator=activator)


FEED_RATE = 0.037
KILL_RATE = 0.06
TIME_STEP = 8.0
SUBSTRATE_DIFFUSION = 4e-7
ACTIVATOR_DIFFUSION = 2e-7


def signed_squares(total):
    indices = jnp.arange(total, dtype=jnp.int32)
    signed = jnp.where(2 * indices < total, indices, indices - total).astype(jnp.float32)
    angular = (2.0 * math.pi) * signed
    return angular * angular


def section_factors(wave_number, diffusion, decay_rate):
    linear = -diffusion * wave_number - decay_rate
    exponent = linear * (0.5 * TIME_STEP)
    return jnp.exp(exponent), jnp.expm1(exponent) / linear


def species_section(field, source, wave_number, diffusion, decay_rate):
    growth, forcing = section_factors(wave_number, diffusion, decay_rate)
    spectrum = jnp.fft.fft2(field + 1j * source)
    advanced = spectrum * (growth - 1j * forcing)
    return jnp.real(jnp.fft.ifft2(advanced)).astype(jnp.float32)


def reference(substrate, activator):
    reaction = substrate * activator * activator
    wave_number = signed_squares(NX)[:, None] + signed_squares(NY)[None, :]
    substrate_section = species_section(substrate, FEED_RATE - reaction, wave_number, SUBSTRATE_DIFFUSION, FEED_RATE)
    activator_section = species_section(activator, reaction, wave_number, ACTIVATOR_DIFFUSION, FEED_RATE + KILL_RATE)
    return (substrate_section, activator_section)
```

```python
import math

import jax
import jax.numpy as jnp
import numpy as np
from jax import lax
from jax.experimental import pallas as pl
from jax.experimental.pallas import tpu as pltpu
from jax.sharding import Mesh
from jax.sharding import PartitionSpec as P

ROW = ("row_0", "row_1", "row_2")
ALL = ("row_0", "row_1", "row_2", "col")

FEED_RATE = 0.037
KILL_RATE = 0.06
TIME_STEP = 8.0
SUBSTRATE_DIFFUSION = 4e-07
ACTIVATOR_DIFFUSION = 2e-07

N = 4096
R = 32
C = 16
I = 8
M = 256
D = R * C
LANES = 128


def add(a, b):
    return b if a is None else a if b is None else a + b


def sub(a, b):
    return (None if b is None else -b) if a is None else a if b is None else a - b


def scale(a, c):
    if a is None or c == 0.0:
        return None
    return a if c == 1.0 else -a if c == -1.0 else a * c


def turn(z, k, n, sign):
    c, s = unit(k, n, sign)
    return sub(scale(z[0], c), scale(z[1], s)), add(scale(z[0], s), scale(z[1], c))


def unit(k, n, sign):
    quarter, rest = divmod(4 * (k % n), n)
    if rest == 0:
        c, s = ((1.0, 0.0), (0.0, 1.0), (-1.0, 0.0), (0.0, -1.0))[quarter]
    else:
        c, s = math.cos(2 * math.pi * k / n), math.sin(2 * math.pi * k / n)
    return c, sign * s


def dft(values, sign):
    n = len(values)
    if n == 1:
        return values
    even, odd = dft(values[0::2], sign), dft(values[1::2], sign)
    odd = [turn(z, k, n, sign) for k, z in enumerate(odd)]
    pairs = list(zip(even, odd))
    return [(add(e[0], o[0]), add(e[1], o[1])) for e, o in pairs] + [
        (sub(e[0], o[0]), sub(e[1], o[1])) for e, o in pairs
    ]


def real_dft(values):
    n = len(values)
    if n == 2:
        return [(add(*values), None), (sub(*values), None)]
    even, odd = real_dft(values[0::2]), real_dft(values[1::2])
    odd = [turn(z, k, n, -1) for k, z in enumerate(odd)]
    low = [(add(e[0], o[0]), add(e[1], o[1])) for e, o in zip(even, odd)]
    high = [(sub(e[0], o[0]), sub(o[1], e[1])) for e, o in zip(even, odd)]
    return low + high[: n // 4][::-1]


def dot(a, b, dims=((1,), (0,))):
    return lax.dot_general(
        a, b, (dims, ((), ())), precision=lax.Precision.HIGHEST, preferred_element_type=jnp.float32
    )


def lane_of(shape):
    return lax.broadcasted_iota(jnp.int32, shape, len(shape) - 1)


def y_forward(fields, cos_y, sin_y, matrix, out, turned):
    for f in range(3):
        lines = []
        for c in range(C):
            if f < 2:
                lines.append(fields[c, f * I : (f + 1) * I, :])
            else:
                a = fields[c, I:, :]
                lines.append(fields[c, :I, :] * a * a)
        half = real_dft(lines)
        for k in range(C):
            re, im = half[k] if k <= C // 2 else half[C - k]
            if im is not None and k > C // 2:
                im = -im
            if k:
                c, s = cos_y[k : k + 1, :], sin_y[k : k + 1, :]
                if im is None:
                    re, im = re * c, -re * s
                else:
                    re, im = re * c + im * s, im * c - re * s
            else:
                im = jnp.zeros_like(re)
            row = k * 32 + f * I
            turned[row : row + I, :M] = re
            turned[row : row + I, M:] = im
    for k in range(C):
        row = k * 32 + 3 * I
        turned[row : row + I, :] = jnp.zeros((I, 2 * M), jnp.float32)
    lane = lane_of((R, LANES))
    for t in range(4):
        half = dot(matrix[...], turned[t * LANES : (t + 1) * LANES, :], ((1,), (1,)))
        for part in range(2):
            blocks = [half[part * 128 + 32 * s : part * 128 + 32 * (s + 1), :] for s in range(4)]
            if t == 0 and part == 1:
                first = (lax.broadcasted_iota(jnp.int32, (R, LANES), 0) == 0) & (lane < 32)
                blocks[0] = jnp.where(first, half[256:257, :], blocks[0])
            for j in range(4):
                piece = None
                for s in range(4):
                    moved = blocks[s] if s == j else pltpu.roll(blocks[s], 32 * (s - j) % LANES, 1)
                    piece = moved if piece is None else jnp.where(lane >= 32 * s, moved, piece)
                out[pl.ds((4 * t + j) * 2 + part, R, stride=2 * C), :] = piece


def x_section(first, lines, cos_c, sin_c, cos_i, sin_i, forward, backward, growth, forcing, out, a_re, a_im, wide):
    for h in range(2):
        values = [
            (
                lines[pl.ds(32 * r + 16 * h, 8, stride=2), :],
                lines[pl.ds(32 * r + 16 * h + 1, 8, stride=2), :],
            )
            for r in range(R)
        ]
        for k, (re, im) in enumerate(dft(values, -1)):
            a_re[k * C + 8 * h : k * C + 8 * h + 8, :] = re
            a_im[k * C + 8 * h : k * C + 8 * h + 8, :] = im
    for h in range(4):
        values = []
        for c in range(C):
            rows = slice(c * R + 8 * h, c * R + 8 * h + 8)
            re, im = a_re[pl.ds(8 * h * C + c, 8, stride=C), :], a_im[pl.ds(8 * h * C + c, 8, stride=C), :]
            u, v = cos_c[rows, :], sin_c[rows, :]
            values.append((re * u + im * v, im * u - re * v))
        for k, (re, im) in enumerate(dft(values, -1)):
            rows = slice(k * R + 8 * h, k * R + 8 * h + 8)
            u, v = cos_i[rows, :], sin_i[rows, :]
            wide[rows, :LANES] = re * u + im * v
            wide[rows, LANES:] = im * u - re * v
    spectra = dot(wide[...], forward[...])
    g, f = growth[...], forcing[...]
    wide[:, :LANES] = g * spectra[:, :LANES] + f * spectra[:, 2 * LANES : 3 * LANES]
    wide[:, LANES:] = g * spectra[:, LANES : 2 * LANES] + f * spectra[:, 3 * LANES :]
    wide[...] = dot(wide[...], backward[...])
    for h in range(4):
        values = []
        for k in range(C):
            rows = slice(k * R + 8 * h, k * R + 8 * h + 8)
            re, im = wide[rows, :LANES], wide[rows, LANES:]
            u, v = cos_i[rows, :], sin_i[rows, :]
            values.append((re * u - im * v, im * u + re * v))
        for c, (re, im) in enumerate(dft(values, 1)):
            rows = slice(c * R + 8 * h, c * R + 8 * h + 8)
            u, v = cos_c[rows, :], sin_c[rows, :]
            a_re[pl.ds(8 * h * C + c, 8, stride=C), :] = re * u - im * v
            a_im[pl.ds(8 * h * C + c, 8, stride=C), :] = im * u + re * v
    lane = lane_of((8, LANES))
    packed = (lane < 80) & (first[0] == 1)
    for h in range(2):
        values = [
            (a_re[k * C + 8 * h : k * C + 8 * h + 8, :], a_im[k * C + 8 * h : k * C + 8 * h + 8, :])
            for k in range(R)
        ]
        for r, (re, im) in enumerate(dft(values, 1)):
            im = jnp.where(packed, im, pltpu.roll(im, 64, 1))
            out[r * C + 8 * h : r * C + 8 * h + 8, :] = jnp.where(lane < 64, re, im)


def y_backward(pieces, constant, cos_y, sin_y, matrix, out, spectrum, turned):
    lane = lane_of((R, LANES))
    for t in range(2):
        sources = [pieces[pl.ds(8 * t + j, R, stride=C), :] for j in range(8)]
        for b in range(8):
            block = None
            for j in range(8):
                moved = sources[j] if j == b else pltpu.roll(sources[j], 16 * (j - b) % LANES, 1)
                block = moved if block is None else jnp.where(lane >= 16 * j, moved, block)
            spectrum[b * R : (b + 1) * R, t * LANES : (t + 1) * LANES] = block
    flipped = spectrum[...].T
    turned[...] = dot(flipped, matrix[...])
    parity = 1.0 - 2.0 * (lane_of((16, M)) % 2).astype(jnp.float32)
    values = []
    for k in range(C):
        re, im = turned[16 * k : 16 * (k + 1), :M], turned[16 * k : 16 * (k + 1), M:]
        if k == 0:
            re, im = re - flipped[:16, 0:1] + flipped[:16, 128:129] * parity, None
        else:
            u, v = cos_y[k : k + 1, :], sin_y[k : k + 1, :]
            re, im = re * u - im * v, im * u + re * v
        values.append((re, im))
    substrate_row = lax.broadcasted_iota(jnp.int32, (16, M), 0) < I
    shift = jnp.where(substrate_row, constant[0], 0.0)
    for c, (re, _) in enumerate(dft(values, 1)):
        out[c] = re + shift


def tables():
    f32 = np.float32
    angle = 2 * np.pi / N * (np.arange(C)[:, None] * np.arange(M)[None, :])
    cos_y, sin_y = np.cos(angle), np.sin(angle)
    turn_m = 2 * np.pi / M * (np.arange(128)[:, None] * np.arange(M)[None, :] % M)
    c, s = np.cos(turn_m), np.sin(turn_m)
    last = np.zeros((8, 2 * M))
    last[0, :M] = 1 - 2 * (np.arange(M) % 2)
    y_matrix = np.concatenate([np.block([[c, s], [-s, c]]), last])
    y_inverse = 2 * np.block([[c, s], [-s, c]])
    k_r = np.tile(np.arange(R), C)
    outer = np.repeat(np.arange(C), R)
    ones = np.ones((1, LANES))
    angle = 2 * np.pi / D * (outer * k_r % D)[:, None] * ones
    cos_c, sin_c = np.cos(angle), np.sin(angle)
    angle = 2 * np.pi / N * ((k_r + R * outer)[:, None] * (np.arange(LANES) % I)[None, :] % N)
    cos_i, sin_i = np.cos(angle), np.sin(angle)
    angle = 2 * np.pi / I * (np.arange(I)[:, None] * np.arange(I)[None, :] % I)
    c, s = np.cos(angle), np.sin(angle)
    forward = np.zeros((2, LANES, 2, 2, LANES))
    backward = np.zeros((2, LANES, 2, LANES))
    for slot in range(5):
        for field in range(2):
            here = slice(16 * slot + I * field, 16 * slot + I * field + I)
            backward[0, here, 0, here], backward[1, here, 0, here] = c, -s
            backward[0, here, 1, here], backward[1, here, 1, here] = s, c
            for kind, taken in enumerate((field, 2)):
                start = 32 * (slot % 4) + I * taken
                there = slice(start, start + I)
                forward[0, there, kind, 0, here], forward[1, there, kind, 0, here] = c, s
                forward[0, there, kind, 1, here], forward[1, there, kind, 1, here] = -s, c
    forward = forward.reshape(2 * LANES, 4 * LANES)
    backward = backward.reshape(2 * LANES, 2 * LANES)
    both = (cos_y, sin_y, y_matrix, y_inverse, cos_c, sin_c, cos_i, sin_i, forward, backward)
    return [a.astype(f32) for a in both]


def signed_squares(wave_index):
    signed = jnp.where(2 * wave_index < N, wave_index, wave_index - N).astype(jnp.float32)
    angular = 2.0 * math.pi * signed
    return angular * angular


def factors(row_index, col_index):
    row = lax.broadcasted_iota(jnp.int32, (D, LANES), 0)
    lane = lane_of((D, LANES))
    p = row % R + R * (row // R) + D * (lane % I)
    slot = lane // 16
    q = jnp.where(slot == 4, N // 2, col_index + C * (R * (slot % 4) + row_index))
    wave_number = signed_squares(p) + signed_squares(q)
    substrate = lane // I % 2 == 0
    diffusion = jnp.where(substrate, SUBSTRATE_DIFFUSION, ACTIVATOR_DIFFUSION)
    decay = jnp.where(substrate, FEED_RATE, FEED_RATE + KILL_RATE)
    linear = -diffusion * wave_number - decay
    exponent = linear * (0.5 * TIME_STEP)
    normalize = 1.0 / (N * N)
    growth = jnp.exp(exponent) * normalize
    forcing = jnp.expm1(exponent) / linear * jnp.where(substrate, -normalize, normalize)
    return growth, forcing


def call(body, out_shape, scratch, *operands, scalars=0):
    spaces = [pl.BlockSpec(memory_space=pltpu.SMEM if k < scalars else pltpu.VMEM) for k in range(len(operands))]
    return pl.pallas_call(
        body,
        out_shape=jax.ShapeDtypeStruct(out_shape, jnp.float32),
        in_specs=spaces,
        out_specs=pl.BlockSpec(memory_space=pltpu.VMEM),
        scratch_shapes=[pltpu.VMEM(shape, jnp.float32) for shape in scratch],
        compiler_params=pltpu.CompilerParams(vmem_limit_bytes=48 * 1024 * 1024),
    )(*operands)


def y_backward_body(constant, pieces, *rest):
    return y_backward(pieces, constant, *rest)


def on_device(substrate, activator):
    cos_y, sin_y, y_matrix, y_inverse, cos_c, sin_c, cos_i, sin_i, forward, backward = tables()
    row_index = lax.axis_index(ROW)
    col_index = lax.axis_index("col")
    growth, forcing = factors(row_index, col_index)
    first = ((row_index == 0) & (col_index == 0)).astype(jnp.int32).reshape(1)
    rate = jnp.full((1,), -FEED_RATE, jnp.float32)
    constant = jnp.expm1(rate * (0.5 * TIME_STEP)) / rate * FEED_RATE

    fields = jnp.concatenate([substrate.reshape(C, I, M), activator.reshape(C, I, M)], axis=1)
    fields = lax.all_to_all(fields, "col", 0, 0, tiled=True)
    pieces = call(y_forward, (2 * D, LANES), [(512, 2 * M)], fields, cos_y, sin_y, y_matrix)
    lines = lax.all_to_all(pieces.reshape(D, 2, LANES), ALL, 0, 0, tiled=True).reshape(2 * D, LANES)
    pieces = call(
        x_section,
        (D, LANES),
        [(D, LANES), (D, LANES), (D, 2 * LANES)],
        first,
        lines,
        cos_c,
        sin_c,
        cos_i,
        sin_i,
        forward,
        backward,
        growth,
        forcing,
        scalars=1,
    )
    pieces = lax.all_to_all(pieces.reshape(D, 1, LANES), ALL, 0, 0, tiled=True).reshape(D, LANES)
    fields = call(
        y_backward_body, (C, 2 * I, M), [(M, M), (M, 2 * M)], constant, pieces, cos_y, sin_y, y_inverse, scalars=1
    )
    fields = lax.all_to_all(fields, "col", 0, 0, tiled=True)
    return (fields[:, :I].reshape(C * I, M), fields[:, I:].reshape(C * I, M))


def solution(mesh):
    split = Mesh(
        mesh.devices.reshape(8, 2, 2, mesh.shape["col"]), ("row_0", "row_1", "row_2", "col")
    )
    placed = (P(ROW, "col"), P(ROW, "col"))
    return jax.shard_map(on_device, mesh=split, in_specs=placed, out_specs=placed, check_vma=False)
```

```python
import math

import jax
import jax.numpy as jnp
import numpy as np
from jax import lax
from jax.experimental import pallas as pl
from jax.experimental.pallas import tpu as pltpu
from jax.sharding import Mesh
from jax.sharding import PartitionSpec as P

ROW = ("row_0", "row_1", "row_2")
ALL = ("row_0", "row_1", "row_2", "col")

FEED_RATE = 0.037
KILL_RATE = 0.06
TIME_STEP = 8.0
SUBSTRATE_DIFFUSION = 4e-07
ACTIVATOR_DIFFUSION = 2e-07

N = 4096
R = 32
C = 16
I = 8
M = 256
D = R * C
LANES = 128


def add(a, b):
    return b if a is None else a if b is None else a + b


def sub(a, b):
    return (None if b is None else -b) if a is None else a if b is None else a - b


def scale(a, c):
    if a is None or c == 0.0:
        return None
    return a if c == 1.0 else -a if c == -1.0 else a * c


def turn(z, k, n, sign):
    c, s = unit(k, n, sign)
    return sub(scale(z[0], c), scale(z[1], s)), add(scale(z[0], s), scale(z[1], c))


def unit(k, n, sign):
    quarter, rest = divmod(4 * (k % n), n)
    if rest == 0:
        c, s = ((1.0, 0.0), (0.0, 1.0), (-1.0, 0.0), (0.0, -1.0))[quarter]
    else:
        c, s = math.cos(2 * math.pi * k / n), math.sin(2 * math.pi * k / n)
    return c, sign * s


def dft(values, sign):
    n = len(values)
    if n == 1:
        return values
    even, odd = dft(values[0::2], sign), dft(values[1::2], sign)
    odd = [turn(z, k, n, sign) for k, z in enumerate(odd)]
    pairs = list(zip(even, odd))
    return [(add(e[0], o[0]), add(e[1], o[1])) for e, o in pairs] + [
        (sub(e[0], o[0]), sub(e[1], o[1])) for e, o in pairs
    ]


def real_dft(values):
    n = len(values)
    if n == 2:
        return [(add(*values), None), (sub(*values), None)]
    even, odd = real_dft(values[0::2]), real_dft(values[1::2])
    odd = [turn(z, k, n, -1) for k, z in enumerate(odd)]
    low = [(add(e[0], o[0]), add(e[1], o[1])) for e, o in zip(even, odd)]
    high = [(sub(e[0], o[0]), sub(o[1], e[1])) for e, o in zip(even, odd)]
    return low + high[: n // 4][::-1]


def halves(a):
    high = a.astype(jnp.bfloat16)
    return high, (a - high.astype(jnp.float32)).astype(jnp.bfloat16)


def dot(a, b, dims=((1,), (0,))):
    def product(u, v):
        return lax.dot_general(u, v, (dims, ((), ())), preferred_element_type=jnp.float32)

    return product(a[0], b[0]) + (product(a[1], b[0]) + product(a[0], b[1]))


def lane_of(shape):
    return lax.broadcasted_iota(jnp.int32, shape, len(shape) - 1)


def y_forward(fields, cos_y, sin_y, high, low, out, turned):
    for f in range(3):
        lines = []
        for c in range(C):
            if f < 2:
                lines.append(fields[c, f * I : (f + 1) * I, :])
            else:
                a = fields[c, I:, :]
                lines.append(fields[c, :I, :] * a * a)
        half = real_dft(lines)
        for k in range(C):
            re, im = half[k] if k <= C // 2 else half[C - k]
            if im is not None and k > C // 2:
                im = -im
            if k:
                c, s = cos_y[k : k + 1, :], sin_y[k : k + 1, :]
                if im is None:
                    re, im = re * c, -re * s
                else:
                    re, im = re * c + im * s, im * c - re * s
            else:
                im = jnp.zeros_like(re)
            row = k * 32 + f * I
            turned[row : row + I, :M] = re
            turned[row : row + I, M:] = im
    for k in range(C):
        row = k * 32 + 3 * I
        turned[row : row + I, :] = jnp.zeros((I, 2 * M), jnp.float32)
    lane = lane_of((R, LANES))
    for t in range(4):
        half = dot((high[...], low[...]), halves(turned[t * LANES : (t + 1) * LANES, :]), ((1,), (1,)))
        for part in range(2):
            blocks = [half[part * 128 + 32 * s : part * 128 + 32 * (s + 1), :] for s in range(4)]
            if t == 0 and part == 1:
                first = (lax.broadcasted_iota(jnp.int32, (R, LANES), 0) == 0) & (lane < 32)
                blocks[0] = jnp.where(first, half[256:257, :], blocks[0])
            for j in range(4):
                piece = None
                for s in range(4):
                    moved = blocks[s] if s == j else pltpu.roll(blocks[s], 32 * (s - j) % LANES, 1)
                    piece = moved if piece is None else jnp.where(lane >= 32 * s, moved, piece)
                out[pl.ds((4 * t + j) * 2 + part, R, stride=2 * C), :] = piece


def x_section(place, lines, cos_c, sin_c, cos_r, sin_r, cos_k, sin_k, fh, fl, bh, bl, out, a_re, a_im, cos_i, sin_i, wide):
    for h in range(2):
        values = [
            (
                lines[pl.ds(32 * r + 16 * h, 8, stride=2), :],
                lines[pl.ds(32 * r + 16 * h + 1, 8, stride=2), :],
            )
            for r in range(R)
        ]
        for k, (re, im) in enumerate(dft(values, -1)):
            a_re[k * C + 8 * h : k * C + 8 * h + 8, :] = re
            a_im[k * C + 8 * h : k * C + 8 * h + 8, :] = im
    for h in range(4):
        values = []
        for c in range(C):
            rows = slice(c * R + 8 * h, c * R + 8 * h + 8)
            re, im = a_re[pl.ds(8 * h * C + c, 8, stride=C), :], a_im[pl.ds(8 * h * C + c, 8, stride=C), :]
            u, v = cos_c[rows, :], sin_c[rows, :]
            values.append((re * u + im * v, im * u - re * v))
        for k, (re, im) in enumerate(dft(values, -1)):
            rows = slice(k * R + 8 * h, k * R + 8 * h + 8)
            u, v = cos_r[8 * h : 8 * h + 8, :], sin_r[8 * h : 8 * h + 8, :]
            if k:
                c, d = cos_k[k : k + 1, :], sin_k[k : k + 1, :]
                u, v = u * c - v * d, u * d + v * c
            cos_i[rows, :], sin_i[rows, :] = u, v
            wide[rows, :LANES] = re * u + im * v
            wide[rows, LANES:] = im * u - re * v
    for t in range(4):
        rows = slice(t * LANES, (t + 1) * LANES)
        spectra = dot(halves(wide[rows, :]), (fh[...], fl[...]))
        g, f = factors(place, t * LANES)
        re = g * spectra[:, :LANES] + f * spectra[:, 2 * LANES : 3 * LANES]
        im = g * spectra[:, LANES : 2 * LANES] + f * spectra[:, 3 * LANES :]
        advanced = halves(jnp.concatenate([re, im], axis=1))
        wide[rows, :] = dot(advanced, (bh[...], bl[...]))
    for h in range(4):
        values = []
        for k in range(C):
            rows = slice(k * R + 8 * h, k * R + 8 * h + 8)
            re, im = wide[rows, :LANES], wide[rows, LANES:]
            u, v = cos_i[rows, :], sin_i[rows, :]
            values.append((re * u - im * v, im * u + re * v))
        for c, (re, im) in enumerate(dft(values, 1)):
            rows = slice(c * R + 8 * h, c * R + 8 * h + 8)
            u, v = cos_c[rows, :], sin_c[rows, :]
            a_re[pl.ds(8 * h * C + c, 8, stride=C), :] = re * u - im * v
            a_im[pl.ds(8 * h * C + c, 8, stride=C), :] = im * u + re * v
    lane = lane_of((8, LANES))
    packed = (lane < 80) & (place[0] + place[1] == 0)
    for h in range(2):
        values = [
            (a_re[k * C + 8 * h : k * C + 8 * h + 8, :], a_im[k * C + 8 * h : k * C + 8 * h + 8, :])
            for k in range(R)
        ]
        for r, (re, im) in enumerate(dft(values, 1)):
            im = jnp.where(packed, im, pltpu.roll(im, 64, 1))
            out[r * C + 8 * h : r * C + 8 * h + 8, :] = jnp.where(lane < 64, re, im)


def y_backward(pieces, cos_y, sin_y, high, low, out, spectrum, turned):
    lane = lane_of((R, LANES))
    for t in range(2):
        sources = [pieces[pl.ds(8 * t + j, R, stride=C), :] for j in range(8)]
        for b in range(8):
            block = None
            for j in range(8):
                moved = sources[j] if j == b else pltpu.roll(sources[j], 16 * (j - b) % LANES, 1)
                block = moved if block is None else jnp.where(lane >= 16 * j, moved, block)
            spectrum[b * R : (b + 1) * R, t * LANES : (t + 1) * LANES] = block
    flipped = spectrum[...].T
    turned[...] = dot(halves(flipped), (high[...], low[...]))
    parity = 1.0 - 2.0 * (lane_of((16, M)) % 2).astype(jnp.float32)
    values = []
    for k in range(C):
        re, im = turned[16 * k : 16 * (k + 1), :M], turned[16 * k : 16 * (k + 1), M:]
        if k == 0:
            re, im = re - flipped[:16, 0:1] + flipped[:16, 128:129] * parity, None
        else:
            u, v = cos_y[k : k + 1, :], sin_y[k : k + 1, :]
            re, im = re * u - im * v, im * u + re * v
        values.append((re, im))
    substrate_row = lax.broadcasted_iota(jnp.int32, (16, M), 0) < I
    constant = math.expm1(-0.5 * FEED_RATE * TIME_STEP) / -FEED_RATE * FEED_RATE
    shift = jnp.where(substrate_row, constant, 0.0)
    for c, (re, _) in enumerate(dft(values, 1)):
        out[c] = re + shift


def tables():
    f32 = np.float32
    angle = 2 * np.pi / N * (np.arange(C)[:, None] * np.arange(M)[None, :])
    cos_y, sin_y = np.cos(angle), np.sin(angle)
    turn_m = 2 * np.pi / M * (np.arange(128)[:, None] * np.arange(M)[None, :] % M)
    c, s = np.cos(turn_m), np.sin(turn_m)
    last = np.zeros((8, 2 * M))
    last[0, :M] = 1 - 2 * (np.arange(M) % 2)
    y_matrix = np.concatenate([np.block([[c, s], [-s, c]]), last])
    y_inverse = 2 * np.block([[c, s], [-s, c]])
    k_r = np.tile(np.arange(R), C)
    outer = np.repeat(np.arange(C), R)
    ones = np.ones((1, LANES))
    angle = 2 * np.pi / D * (outer * k_r % D)[:, None] * ones
    cos_c, sin_c = np.cos(angle), np.sin(angle)
    lane_i = (np.arange(LANES) % I)[None, :]
    angle = 2 * np.pi / N * (np.arange(R)[:, None] * lane_i)
    cos_r, sin_r = np.cos(angle), np.sin(angle)
    angle = 2 * np.pi / 128 * (np.arange(C)[:, None] * lane_i % 128)
    cos_k, sin_k = np.cos(angle), np.sin(angle)
    angle = 2 * np.pi / I * (np.arange(I)[:, None] * np.arange(I)[None, :] % I)
    c, s = np.cos(angle), np.sin(angle)
    forward = np.zeros((2, LANES, 2, 2, LANES))
    backward = np.zeros((2, LANES, 2, LANES))
    for slot in range(5):
        for field in range(2):
            here = slice(16 * slot + I * field, 16 * slot + I * field + I)
            backward[0, here, 0, here], backward[1, here, 0, here] = c, -s
            backward[0, here, 1, here], backward[1, here, 1, here] = s, c
            for kind, taken in enumerate((field, 2)):
                start = 32 * (slot % 4) + I * taken
                there = slice(start, start + I)
                forward[0, there, kind, 0, here], forward[1, there, kind, 0, here] = c, s
                forward[0, there, kind, 1, here], forward[1, there, kind, 1, here] = -s, c
    forward = forward.reshape(2 * LANES, 4 * LANES)
    backward = backward.reshape(2 * LANES, 2 * LANES)
    def parts(matrix):
        high = matrix.astype(np.float32).astype(jnp.bfloat16)
        return high, (matrix - high.astype(np.float64)).astype(jnp.bfloat16)

    along_y = [a.astype(f32) for a in (cos_y, sin_y)]
    along_x = [a.astype(f32) for a in (cos_c, sin_c, cos_r, sin_r, cos_k, sin_k)]
    return (
        (*along_y, *parts(y_matrix)),
        (*along_x, *parts(forward), *parts(backward)),
        (*along_y, *parts(y_inverse)),
    )


def signed_squares(wave_index):
    signed = jnp.where(2 * wave_index < N, wave_index, wave_index - N).astype(jnp.float32)
    angular = 2.0 * math.pi * signed
    return angular * angular


def factors(place, start):
    row = start + lax.broadcasted_iota(jnp.int32, (LANES, LANES), 0)
    lane = lane_of((1, LANES))
    p = row + D * (lane & (I - 1))
    slot = lane >> 4
    q = jnp.where(slot == 4, N // 2, place[1] + C * (R * (slot & 3) + place[0]))
    wave_number = signed_squares(p) + signed_squares(q)
    substrate = (lane & I) == 0
    diffusion = jnp.where(substrate, SUBSTRATE_DIFFUSION, ACTIVATOR_DIFFUSION)
    decay = jnp.where(substrate, FEED_RATE, FEED_RATE + KILL_RATE)
    linear = -diffusion * wave_number - decay
    grown = jnp.exp(linear * (0.5 * TIME_STEP))
    normalize = 1.0 / (N * N)
    return grown * normalize, (grown - 1.0) / linear * jnp.where(substrate, -normalize, normalize)


def call(body, out_shape, scratch, *operands, scalars=0):
    spaces = [pl.BlockSpec(memory_space=pltpu.SMEM if k < scalars else pltpu.VMEM) for k in range(len(operands))]
    return pl.pallas_call(
        body,
        out_shape=jax.ShapeDtypeStruct(out_shape, jnp.float32),
        in_specs=spaces,
        out_specs=pl.BlockSpec(memory_space=pltpu.VMEM),
        scratch_shapes=[pltpu.VMEM(shape, jnp.float32) for shape in scratch],
        compiler_params=pltpu.CompilerParams(vmem_limit_bytes=48 * 1024 * 1024),
    )(*operands)


def on_device(substrate, activator):
    along_y, along_x, back_y = tables()
    place = jnp.stack([lax.axis_index(ROW), lax.axis_index("col")])
    fields = jnp.concatenate([substrate.reshape(C, I, M), activator.reshape(C, I, M)], axis=1)
    fields, place = lax.optimization_barrier((fields, place))
    fields = lax.all_to_all(fields, "col", 0, 0, tiled=True)
    pieces = call(y_forward, (2 * D, LANES), [(D, 2 * M)], fields, *along_y)
    lines = lax.all_to_all(pieces.reshape(D, 2, LANES), ALL, 0, 0, tiled=True).reshape(2 * D, LANES)
    scratch = [(D, LANES)] * 4 + [(D, 2 * LANES)]
    pieces = call(x_section, (D, LANES), scratch, place, lines, *along_x, scalars=1)
    pieces = lax.all_to_all(pieces.reshape(D, 1, LANES), ALL, 0, 0, tiled=True).reshape(D, LANES)
    fields = call(y_backward, (C, 2 * I, M), [(M, M), (M, 2 * M)], pieces, *back_y)
    fields = lax.all_to_all(fields, "col", 0, 0, tiled=True)
    return (fields[:, :I].reshape(C * I, M), fields[:, I:].reshape(C * I, M))


def solution(mesh):
    split = Mesh(
        mesh.devices.reshape(8, 2, 2, mesh.shape["col"]), ("row_0", "row_1", "row_2", "col")
    )
    placed = (P(ROW, "col"), P(ROW, "col"))
    return jax.shard_map(on_device, mesh=split, in_specs=placed, out_specs=placed, check_vma=False)
```

```python
import math

import jax
import jax.numpy as jnp
import numpy as np
from jax import lax
from jax.experimental import pallas as pl
from jax.experimental.pallas import tpu as pltpu
from jax.sharding import Mesh
from jax.sharding import PartitionSpec as P

ROW = ("row_0", "row_1", "row_2")
ALL = ("row_0", "row_1", "row_2", "col")

FEED_RATE = 0.037
KILL_RATE = 0.06
TIME_STEP = 8.0
SUBSTRATE_DIFFUSION = 4e-07
ACTIVATOR_DIFFUSION = 2e-07

N = 4096
R = 32
C = 16
I = 8
M = 256
D = R * C
LANES = 128


def add(a, b):
    return b if a is None else a if b is None else a + b


def sub(a, b):
    return (None if b is None else -b) if a is None else a if b is None else a - b


def scale(a, c):
    if a is None or c == 0.0:
        return None
    return a if c == 1.0 else -a if c == -1.0 else a * c


def turn(z, k, n, sign):
    c, s = unit(k, n, sign)
    return sub(scale(z[0], c), scale(z[1], s)), add(scale(z[0], s), scale(z[1], c))


def unit(k, n, sign):
    quarter, rest = divmod(4 * (k % n), n)
    if rest == 0:
        c, s = ((1.0, 0.0), (0.0, 1.0), (-1.0, 0.0), (0.0, -1.0))[quarter]
    else:
        c, s = math.cos(2 * math.pi * k / n), math.sin(2 * math.pi * k / n)
    return c, sign * s


def dft(values, sign):
    n = len(values)
    if n == 1:
        return values
    even, odd = dft(values[0::2], sign), dft(values[1::2], sign)
    odd = [turn(z, k, n, sign) for k, z in enumerate(odd)]
    pairs = list(zip(even, odd))
    return [(add(e[0], o[0]), add(e[1], o[1])) for e, o in pairs] + [
        (sub(e[0], o[0]), sub(e[1], o[1])) for e, o in pairs
    ]


def real_dft(values):
    n = len(values)
    if n == 2:
        return [(add(*values), None), (sub(*values), None)]
    even, odd = real_dft(values[0::2]), real_dft(values[1::2])
    odd = [turn(z, k, n, -1) for k, z in enumerate(odd)]
    low = [(add(e[0], o[0]), add(e[1], o[1])) for e, o in zip(even, odd)]
    high = [(sub(e[0], o[0]), sub(o[1], e[1])) for e, o in zip(even, odd)]
    return low + high[: n // 4][::-1]


def halves(a):
    high = a.astype(jnp.bfloat16)
    return high, (a - high.astype(jnp.float32)).astype(jnp.bfloat16)


def dot(a, b, dims=((1,), (0,))):
    def product(u, v):
        return lax.dot_general(u, v, (dims, ((), ())), preferred_element_type=jnp.float32)

    return product(a[0], b[0]) + (product(a[1], b[0]) + product(a[0], b[1]))


def lane_of(shape):
    return lax.broadcasted_iota(jnp.int32, shape, len(shape) - 1)


def by_block(sources, width, lane):
    piece = sources[0]
    for k, source in enumerate(sources[1:], 1):
        piece = jnp.where(lane >= width * k, source, piece)
    return piece


def y_forward(fields, cos_y, sin_y, high, low, out, turned):
    for f in range(3):
        lines = []
        for c in range(C):
            if f < 2:
                lines.append(fields[c, f * I : (f + 1) * I, :])
            else:
                a = fields[c, I:, :]
                lines.append(fields[c, :I, :] * a * a)
        half = real_dft(lines)
        for k in range(C):
            re, im = half[k] if k <= C // 2 else half[C - k]
            if im is not None and k > C // 2:
                im = -im
            if k:
                c, s = cos_y[k : k + 1, :], sin_y[k : k + 1, :]
                if im is None:
                    re, im = re * c, -re * s
                else:
                    re, im = re * c + im * s, im * c - re * s
            else:
                im = jnp.zeros_like(re)
            row = k * 32 + f * I
            turned[row : row + I, :M] = re
            turned[row : row + I, M:] = im
    for k in range(C):
        row = k * 32 + 3 * I
        turned[row : row + I, :] = jnp.zeros((I, 2 * M), jnp.float32)
    parity = 1.0 - 2.0 * (lane_of((I, M)) & 1).astype(jnp.float32)
    place = lane_of((I, LANES))
    last = jnp.zeros((I, LANES), jnp.float32)
    for f in range(3):
        total = jnp.sum(turned[f * I : (f + 1) * I, :M] * parity, axis=1, keepdims=True)
        last = jnp.where(place == 32 * f, total, last)
    lane = lane_of((R, LANES))
    for t in range(4):
        spectra = dot(halves(turned[t * LANES : (t + 1) * LANES, :]), (high[...], low[...]))
        for part in range(2):
            half = spectra[:, part * LANES : (part + 1) * LANES]
            if t == 0 and part == 0:
                half = jnp.concatenate([half[: 3 * I], last, half[4 * I :]], axis=0)
            half = half.T
            blocks = [half[32 * s : 32 * (s + 1), :] for s in range(4)]
            blocks = [blocks[0]] + [pltpu.roll(blocks[s], 32 * s, 1) for s in range(1, 4)]
            for j in range(4):
                piece = by_block([blocks[(k - j) % 4] for k in range(4)], 32, lane)
                out[pl.ds((4 * t + j) * 2 + part, R, stride=2 * C), :] = piece


def swapped(z):
    return pltpu.roll(z, 64, 1)


def packed_dft(values, signs):
    n = len(values)
    if n == 1:
        return values
    even, odd = packed_dft(values[0::2], signs), packed_dft(values[1::2], signs)
    for k in range(1, n // 2):
        c, s = unit(k, n, 1)
        turned = swapped(odd[k]) * (signs if s == 1.0 else signs * s)
        odd[k] = turned if c == 0.0 else odd[k] * c + turned
    return [e + o for e, o in zip(even, odd)] + [e - o for e, o in zip(even, odd)]


def x_section(
    place, lines, cos_c, sin_c, cos_r, sin_r, cos_k, sin_k, decay, fh, fl, bh, bl, out, a_re, a_im, cos_i, sin_i, wide
):
    back = (LANES - 32 * (place[1] & 3)) & (LANES - 1)
    for h in range(2):
        values = [
            tuple(
                pltpu.roll(lines[pl.ds(32 * r + 16 * h + part, 8, stride=2), :], back, 1) for part in range(2)
            )
            for r in range(R)
        ]
        for k, (re, im) in enumerate(dft(values, -1)):
            a_re[k * C + 8 * h : k * C + 8 * h + 8, :] = re
            a_im[k * C + 8 * h : k * C + 8 * h + 8, :] = im
    signs = jnp.where(lane_of((8, LANES)) < 64, -1.0, 1.0)
    for h in range(4):
        values = []
        for c in range(C):
            rows = slice(c * R + 8 * h, c * R + 8 * h + 8)
            re, im = a_re[pl.ds(8 * h * C + c, 8, stride=C), :], a_im[pl.ds(8 * h * C + c, 8, stride=C), :]
            if c:
                u, v = cos_c[rows, :], sin_c[rows, :]
                re, im = re * u + im * v, im * u - re * v
            values.append((re, im))
        for k, (re, im) in enumerate(dft(values, -1)):
            rows = slice(k * R + 8 * h, k * R + 8 * h + 8)
            u, v = cos_r[8 * h : 8 * h + 8, :], sin_r[8 * h : 8 * h + 8, :]
            if k:
                c, d = cos_k[k : k + 1, :], sin_k[k : k + 1, :]
                u, v = u * c - v * d, u * d + v * c
            cos_i[rows, :], sin_i[rows, :] = u, v * signs
            wide[rows, :LANES] = re * u + im * v
            wide[rows, LANES:] = im * u - re * v
    along_y, normal = column_factors(place)
    for t in range(4):
        rows = slice(t * LANES, (t + 1) * LANES)
        spectra = dot(halves(wide[rows, :]), (fh[...], fl[...]))
        linear = decay[rows, :] + along_y
        grown = jnp.exp(linear * (0.5 * TIME_STEP))
        g, f = grown * (1.0 / (N * N)), (grown - 1.0) / linear * normal
        re = g * spectra[:, :LANES] + f * spectra[:, 2 * LANES : 3 * LANES]
        im = g * spectra[:, LANES : 2 * LANES] + f * spectra[:, 3 * LANES :]
        advanced = halves(jnp.concatenate([re, im], axis=1))
        wide[rows, :LANES] = dot(advanced, (bh[...], bl[...]))
    for h in range(4):
        values = []
        for k in range(C):
            rows = slice(k * R + 8 * h, k * R + 8 * h + 8)
            z = wide[rows, :LANES]
            values.append(z * cos_i[rows, :] + swapped(z) * sin_i[rows, :])
        for c, z in enumerate(packed_dft(values, signs)):
            rows = slice(c * R + 8 * h, c * R + 8 * h + 8)
            if c:
                z = z * cos_c[rows, :] + swapped(z) * (sin_c[rows, :] * signs)
            a_re[pl.ds(8 * h * C + c, 8, stride=C), :] = z
    on = 16 * (place[1] & 7)
    for h in range(2):
        values = [a_re[k * C + 8 * h : k * C + 8 * h + 8, :] for k in range(R)]
        for r, z in enumerate(packed_dft(values, signs)):
            out[r * C + 8 * h : r * C + 8 * h + 8, :] = pltpu.roll(z, on, 1)


def y_backward(pieces, cos_y, sin_y, high, low, out, spectrum, turned):
    lane = lane_of((R, LANES))
    for t in range(2):
        sources = [pieces[pl.ds(8 * t + j, R, stride=C), :] for j in range(8)]
        for b in range(8):
            block = by_block([sources[(k - b) % 8] for k in range(8)], 16, lane)
            block = pltpu.roll(block, LANES - 16 * b, 1) if b else block
            spectrum[b * R : (b + 1) * R, t * LANES : (t + 1) * LANES] = block
    flipped = spectrum[...].T
    turned[...] = dot(halves(flipped), (high[...], low[...]))
    parity = 1.0 - 2.0 * (lane_of((16, M)) & 1).astype(jnp.float32)
    values = []
    for k in range(C):
        re, im = turned[16 * k : 16 * (k + 1), :M], turned[16 * k : 16 * (k + 1), M:]
        if k == 0:
            re, im = re - flipped[:16, 0:1] + flipped[:16, 128:129] * parity, None
        else:
            u, v = cos_y[k : k + 1, :], sin_y[k : k + 1, :]
            re, im = re * u - im * v, im * u + re * v
        values.append((re, im))
    substrate_row = lax.broadcasted_iota(jnp.int32, (16, M), 0) < I
    constant = math.expm1(-0.5 * FEED_RATE * TIME_STEP) / -FEED_RATE * FEED_RATE
    shift = jnp.where(substrate_row, constant, 0.0)
    for c, (re, _) in enumerate(dft(values, 1)):
        out[c] = re + shift


def tables():
    f32 = np.float32
    angle = 2 * np.pi / N * (np.arange(C)[:, None] * np.arange(M)[None, :])
    cos_y, sin_y = np.cos(angle), np.sin(angle)
    turn_m = 2 * np.pi / M * (np.arange(M)[:, None] * np.arange(128)[None, :] % M)
    c, s = np.cos(turn_m), np.sin(turn_m)
    y_matrix = np.block([[c, -s], [s, c]])
    y_inverse = 2 * np.block([[c.T, s.T], [-s.T, c.T]])
    k_r = np.tile(np.arange(R), C)
    outer = np.repeat(np.arange(C), R)
    ones = np.ones((1, LANES))
    angle = 2 * np.pi / D * (outer * k_r % D)[:, None] * ones
    cos_c, sin_c = np.cos(angle), np.sin(angle)
    lane_i = (np.arange(LANES) % I)[None, :]
    angle = 2 * np.pi / N * (np.arange(R)[:, None] * lane_i)
    cos_r, sin_r = np.cos(angle), np.sin(angle)
    angle = 2 * np.pi / 128 * (np.arange(C)[:, None] * lane_i % 128)
    cos_k, sin_k = np.cos(angle), np.sin(angle)
    angle = 2 * np.pi / I * (np.arange(I)[:, None] * np.arange(I)[None, :] % I)
    c, s = np.cos(angle), np.sin(angle)
    forward = np.zeros((2, LANES, 2, 2, LANES))
    backward = np.zeros((2, LANES, LANES))
    for slot in range(5):
        for field in range(2):
            here = slice(16 * slot + I * field, 16 * slot + I * field + I)
            if slot < 4:
                there = slice(64 + here.start, 64 + here.stop)
                backward[0, here, here], backward[1, here, here] = c, -s
                backward[0, here, there], backward[1, here, there] = s, c
            else:
                start = slice(I * field, I * field + I)
                there = slice(64 + I * field, 64 + I * field + I)
                backward[0, here, start], backward[1, here, start] = -s, -c
                backward[0, here, there], backward[1, here, there] = c, -s
            for kind, taken in enumerate((field, 2)):
                start = 32 * slot + I * taken if slot < 4 else 32 * taken + 3 * I
                there = slice(start, start + I)
                forward[0, there, kind, 0, here], forward[1, there, kind, 0, here] = c, s
                forward[0, there, kind, 1, here], forward[1, there, kind, 1, here] = -s, c
    forward = forward.reshape(2 * LANES, 4 * LANES)
    backward = backward.reshape(2 * LANES, LANES)
    lane = np.arange(LANES)[None, :]
    p = np.arange(D)[:, None] + D * (lane % I)
    angular = 2 * np.pi * np.where(2 * p < N, p, p - N)
    decay = -np.where(lane // I % 2 == 0, SUBSTRATE_DIFFUSION, ACTIVATOR_DIFFUSION) * angular**2

    def parts(matrix):
        high = matrix.astype(np.float32).astype(jnp.bfloat16)
        return high, (matrix - high.astype(np.float64)).astype(jnp.bfloat16)

    along_y = [a.astype(f32) for a in (cos_y, sin_y)]
    along_x = [a.astype(f32) for a in (cos_c, sin_c, cos_r, sin_r, cos_k, sin_k, decay)]
    return (
        (*along_y, *parts(y_matrix)),
        (*along_x, *parts(forward), *parts(backward)),
        (*along_y, *parts(y_inverse)),
    )


def column_factors(place):
    lane = lane_of((1, LANES))
    slot = lane >> 4
    q = jnp.where(slot == 4, N // 2, place[1] + C * (R * (slot & 3) + place[0]))
    signed = jnp.where(2 * q < N, q, q - N).astype(jnp.float32)
    angular = 2.0 * math.pi * signed
    substrate = (lane & I) == 0
    diffusion = jnp.where(substrate, SUBSTRATE_DIFFUSION, ACTIVATOR_DIFFUSION)
    decay = jnp.where(substrate, FEED_RATE, FEED_RATE + KILL_RATE)
    normalize = 1.0 / (N * N)
    return -diffusion * (angular * angular) - decay, jnp.where(substrate, -normalize, normalize)


def call(body, out_shape, scratch, *operands, scalars=0):
    spaces = [pl.BlockSpec(memory_space=pltpu.SMEM if k < scalars else pltpu.VMEM) for k in range(len(operands))]
    return pl.pallas_call(
        body,
        out_shape=jax.ShapeDtypeStruct(out_shape, jnp.float32),
        in_specs=spaces,
        out_specs=pl.BlockSpec(memory_space=pltpu.VMEM),
        scratch_shapes=[pltpu.VMEM(shape, jnp.float32) for shape in scratch],
        compiler_params=pltpu.CompilerParams(vmem_limit_bytes=48 * 1024 * 1024),
    )(*operands)


def on_device(substrate, activator):
    along_y, along_x, back_y = tables()
    place = jnp.stack([lax.axis_index(ROW), lax.axis_index("col")])
    fields = jnp.concatenate([substrate.reshape(C, I, M), activator.reshape(C, I, M)], axis=1)
    fields, place = lax.optimization_barrier((fields, place))
    fields = lax.all_to_all(fields, "col", 0, 0, tiled=True)
    pieces = call(y_forward, (2 * D, LANES), [(D, 2 * M)], fields, *along_y)
    lines = lax.all_to_all(pieces.reshape(D, 2, LANES), ALL, 0, 0, tiled=True).reshape(2 * D, LANES)
    scratch = [(D, LANES)] * 4 + [(D, 2 * LANES)]
    pieces = call(x_section, (D, LANES), scratch, place, lines, *along_x, scalars=1)
    pieces = lax.all_to_all(pieces.reshape(D, 1, LANES), ALL, 0, 0, tiled=True).reshape(D, LANES)
    fields = call(y_backward, (C, 2 * I, M), [(M, M), (M, 2 * M)], pieces, *back_y)
    fields = lax.all_to_all(fields, "col", 0, 0, tiled=True)
    return (fields[:, :I].reshape(C * I, M), fields[:, I:].reshape(C * I, M))


def solution(mesh):
    split = Mesh(
        mesh.devices.reshape(8, 2, 2, mesh.shape["col"]), ("row_0", "row_1", "row_2", "col")
    )
    placed = (P(ROW, "col"), P(ROW, "col"))
    return jax.shard_map(on_device, mesh=split, in_specs=placed, out_specs=placed, check_vma=False)
```

```python
import math

import jax
import jax.numpy as jnp
import numpy as np
from jax import lax
from jax.experimental import pallas as pl
from jax.experimental.pallas import tpu as pltpu
from jax.sharding import Mesh
from jax.sharding import PartitionSpec as P

ROW = ("row_0", "row_1", "row_2")
ALL = ("row_0", "row_1", "row_2", "col")

FEED_RATE = 0.037
KILL_RATE = 0.06
TIME_STEP = 8.0
SUBSTRATE_DIFFUSION = 4e-07
ACTIVATOR_DIFFUSION = 2e-07

N = 4096
R = 32
C = 16
I = 8
M = 256
D = R * C
LANES = 128


def add(a, b):
    return b if a is None else a if b is None else a + b


def sub(a, b):
    return (None if b is None else -b) if a is None else a if b is None else a - b


def scale(a, c):
    if a is None or c == 0.0:
        return None
    return a if c == 1.0 else -a if c == -1.0 else a * c


def turn(z, k, n, sign):
    c, s = unit(k, n, sign)
    return sub(scale(z[0], c), scale(z[1], s)), add(scale(z[0], s), scale(z[1], c))


def unit(k, n, sign):
    quarter, rest = divmod(4 * (k % n), n)
    if rest == 0:
        c, s = ((1.0, 0.0), (0.0, 1.0), (-1.0, 0.0), (0.0, -1.0))[quarter]
    else:
        c, s = math.cos(2 * math.pi * k / n), math.sin(2 * math.pi * k / n)
    return c, sign * s


def dft(values, sign):
    n = len(values)
    if n == 1:
        return values
    even, odd = dft(values[0::2], sign), dft(values[1::2], sign)
    odd = [turn(z, k, n, sign) for k, z in enumerate(odd)]
    pairs = list(zip(even, odd))
    return [(add(e[0], o[0]), add(e[1], o[1])) for e, o in pairs] + [
        (sub(e[0], o[0]), sub(e[1], o[1])) for e, o in pairs
    ]


def real_dft(values):
    n = len(values)
    if n == 2:
        return [(add(*values), None), (sub(*values), None)]
    even, odd = real_dft(values[0::2]), real_dft(values[1::2])
    odd = [turn(z, k, n, -1) for k, z in enumerate(odd)]
    low = [(add(e[0], o[0]), add(e[1], o[1])) for e, o in zip(even, odd)]
    high = [(sub(e[0], o[0]), sub(o[1], e[1])) for e, o in zip(even, odd)]
    return low + high[: n // 4][::-1]


def halves(a):
    high = a.astype(jnp.bfloat16)
    return high, (a - high.astype(jnp.float32)).astype(jnp.bfloat16)


def dot(a, b, dims=((1,), (0,))):
    def product(u, v):
        return lax.dot_general(u, v, (dims, ((), ())), preferred_element_type=jnp.float32)

    return product(a[0], b[0]) + (product(a[1], b[0]) + product(a[0], b[1]))


def lane_of(shape):
    return lax.broadcasted_iota(jnp.int32, shape, len(shape) - 1)


def by_block(sources, width, lane):
    piece = sources[0]
    for k, source in enumerate(sources[1:], 1):
        piece = jnp.where(lane >= width * k, source, piece)
    return piece


def y_forward(fields, cos_y, sin_y, high, low, out, turned):
    for f in range(3):
        lines = []
        for c in range(C):
            if f < 2:
                lines.append(fields[c, f * I : (f + 1) * I, :])
            else:
                a = fields[c, I:, :]
                lines.append(fields[c, :I, :] * a * a)
        half = real_dft(lines)
        for k in range(C):
            re, im = half[k] if k <= C // 2 else half[C - k]
            if im is not None and k > C // 2:
                im = -im
            if k:
                c, s = cos_y[k : k + 1, :], sin_y[k : k + 1, :]
                if im is None:
                    re, im = re * c, -re * s
                else:
                    re, im = re * c + im * s, im * c - re * s
            else:
                im = jnp.zeros_like(re)
            row = k * 32 + f * I
            turned[row : row + I, :M] = re
            turned[row : row + I, M:] = im
    for k in range(C):
        row = k * 32 + 3 * I
        turned[row : row + I, :] = jnp.zeros((I, 2 * M), jnp.float32)
    parity = 1.0 - 2.0 * (lane_of((I, M)) & 1).astype(jnp.float32)
    place = lane_of((I, LANES))
    last = jnp.zeros((I, LANES), jnp.float32)
    for f in range(3):
        total = jnp.sum(turned[f * I : (f + 1) * I, :M] * parity, axis=1, keepdims=True)
        last = jnp.where(place == 32 * f, total, last)
    lane = lane_of((R, LANES))
    for t in range(4):
        spectra = dot(halves(turned[t * LANES : (t + 1) * LANES, :]), (high[...], low[...]))
        for part in range(2):
            half = spectra[:, part * LANES : (part + 1) * LANES]
            if t == 0 and part == 0:
                half = jnp.concatenate([half[: 3 * I], last, half[4 * I :]], axis=0)
            half = half.T
            blocks = [half[32 * s : 32 * (s + 1), :] for s in range(4)]
            blocks = [blocks[0]] + [pltpu.roll(blocks[s], 32 * s, 1) for s in range(1, 4)]
            for j in range(4):
                piece = by_block([blocks[(k - j) % 4] for k in range(4)], 32, lane)
                out[pl.ds((4 * t + j) * 2 + part, R, stride=2 * C), :] = piece


def x_section(
    place, lines, cos_c, sin_c, cos_r, sin_r, cos_k, sin_k, decay, fh, fl, bh, bl, out, a_re, a_im, cos_i, sin_i, wide, gh, gl, late_c, late_s
):
    for part in range(2):
        for slot in range(4):
            here = slice(LANES * part + 32 * slot, LANES * part + 32 * (slot + 1))
            there = pl.ds(pl.multiple_of(LANES * part + 32 * ((slot + place[1]) & 3), 32), 32)
            gh[there, :] = fh[here, :]
            gl[there, :] = fl[here, :]
    for h in range(2):
        values = [
            tuple(lines[pl.ds(32 * r + 16 * h + part, 8, stride=2), :] for part in range(2)) for r in range(R)
        ]
        for k, (re, im) in enumerate(dft(values, -1)):
            a_re[k * 24 + 8 * h : k * 24 + 8 * h + 8, :] = re
            a_im[k * 24 + 8 * h : k * 24 + 8 * h + 8, :] = im

    def turn_c(c, h):
        rows = slice((c - 1) * R + 8 * h, (c - 1) * R + 8 * h + 8)
        if c <= 8:
            return cos_c[rows, :], sin_c[rows, :]
        rows = slice((c - 9) * R + 8 * h, (c - 9) * R + 8 * h + 8)
        return late_c[rows, :], late_s[rows, :]

    for h in range(4):
        values = []
        for c in range(C):
            re, im = a_re[pl.ds(8 * h * 24 + c, 8, stride=24), :], a_im[pl.ds(8 * h * 24 + c, 8, stride=24), :]
            if c > 8:
                (u, v), (w, z) = turn_c(c - 8, h), turn_c(8, h)
                rows = slice((c - 9) * R + 8 * h, (c - 9) * R + 8 * h + 8)
                late_c[rows, :], late_s[rows, :] = u * w - v * z, u * z + v * w
            if c:
                u, v = turn_c(c, h)
                re, im = re * u + im * v, im * u - re * v
            values.append((re, im))
        for k, (re, im) in enumerate(dft(values, -1)):
            rows = slice(h * LANES + 8 * k, h * LANES + 8 * k + 8)
            u, v = cos_r[8 * h : 8 * h + 8, :], sin_r[8 * h : 8 * h + 8, :]
            if k:
                c, d = cos_k[k : k + 1, :], sin_k[k : k + 1, :]
                u, v = u * c - v * d, u * d + v * c
            cos_i[rows, :], sin_i[rows, :] = u, v
            wide[rows, :LANES] = re * u + im * v
            wide[rows, LANES:] = im * u - re * v
    along_y, normal = column_factors(place)
    low_lanes = lane_of((8, LANES)) < 64
    for g in range(2):
        advanced = []
        for h in (2 * g, 2 * g + 1):
            rows = slice(h * LANES, (h + 1) * LANES)
            spectra = dot(halves(wide[rows, :]), (gh[...], gl[...]))
            linear = decay[rows, :] + along_y
            grown = jnp.exp(linear * (0.5 * TIME_STEP))
            growth, forcing = grown * (1.0 / (N * N)), (grown - 1.0) / linear * normal
            advanced.append(growth * spectra[:, :LANES] + forcing * spectra[:, 2 * LANES : 3 * LANES])
            advanced.append(growth * spectra[:, LANES : 2 * LANES] + forcing * spectra[:, 3 * LANES :])
        both = dot(halves(jnp.concatenate(advanced, axis=1)), (bh[...], bl[...]))
        values = []
        for k in range(C):
            rows = [slice(h * LANES + 8 * k, h * LANES + 8 * k + 8) for h in (2 * g, 2 * g + 1)]
            u, v = (jnp.where(low_lanes, t[rows[0], :], t[rows[1], :]) for t in (cos_i, sin_i))
            re, im = both[8 * k : 8 * k + 8, :LANES], both[8 * k : 8 * k + 8, LANES:]
            values.append((re * u - im * v, im * u + re * v))
        values = dft(values, 1)
        for c in range(1, C):
            first, second = turn_c(c, 2 * g), turn_c(c, 2 * g + 1)
            u, v = jnp.where(low_lanes, first[0], second[0]), jnp.where(low_lanes, first[1], second[1])
            re, im = values[c]
            values[c] = re * u - im * v, im * u + re * v
        for c in range(8):
            for part, kept in enumerate((a_re, a_im)):
                one, two = values[c][part], values[c + 8][part]
                kept[pl.ds(128 * g + c, 8, stride=8), :] = jnp.where(low_lanes, one, pltpu.roll(two, 64, 1))
                kept[pl.ds(128 * g + 64 + c, 8, stride=8), :] = jnp.where(low_lanes, pltpu.roll(one, 64, 1), two)
    on = 16 * (place[1] & 7)
    values = [(a_re[8 * k : 8 * k + 8, :], a_im[8 * k : 8 * k + 8, :]) for k in range(R)]
    for r, (re, im) in enumerate(dft(values, 1)):
        one = jnp.where(low_lanes, re, pltpu.roll(im, 64, 1))
        two = jnp.where(low_lanes, pltpu.roll(re, 64, 1), im)
        out[r * C : r * C + 8, :] = pltpu.roll(one, on, 1)
        out[r * C + 8 : r * C + 16, :] = pltpu.roll(two, on, 1)


def y_backward(pieces, cos_y, sin_y, high, low, out, spectrum, turned):
    lane = lane_of((R, LANES))
    for t in range(2):
        sources = [pieces[pl.ds(8 * t + j, R, stride=C), :] for j in range(8)]
        for b in range(8):
            block = by_block([sources[(k - b) % 8] for k in range(8)], 16, lane)
            block = pltpu.roll(block, LANES - 16 * b, 1) if b else block
            spectrum[b * R : (b + 1) * R, t * LANES : (t + 1) * LANES] = block
    flipped = spectrum[...].T
    turned[...] = dot(halves(flipped), (high[...], low[...]))
    parity = 1.0 - 2.0 * (lane_of((16, M)) & 1).astype(jnp.float32)
    values = []
    for k in range(C):
        re, im = turned[16 * k : 16 * (k + 1), :M], turned[16 * k : 16 * (k + 1), M:]
        if k == 0:
            re, im = re - flipped[:16, 0:1] + flipped[:16, 128:129] * parity, None
        else:
            u, v = cos_y[k : k + 1, :], sin_y[k : k + 1, :]
            re, im = re * u - im * v, im * u + re * v
        values.append((re, im))
    substrate_row = lax.broadcasted_iota(jnp.int32, (16, M), 0) < I
    constant = math.expm1(-0.5 * FEED_RATE * TIME_STEP) / -FEED_RATE * FEED_RATE
    shift = jnp.where(substrate_row, constant, 0.0)
    for c, (re, _) in enumerate(dft(values, 1)):
        out[c] = re + shift


def tables():
    f32 = np.float32
    angle = 2 * np.pi / N * (np.arange(C)[:, None] * np.arange(M)[None, :])
    cos_y, sin_y = np.cos(angle), np.sin(angle)
    turn_m = 2 * np.pi / M * (np.arange(M)[:, None] * np.arange(128)[None, :] % M)
    c, s = np.cos(turn_m), np.sin(turn_m)
    y_matrix = np.block([[c, -s], [s, c]])
    y_inverse = 2 * np.block([[c.T, s.T], [-s.T, c.T]])
    ones = np.ones((1, LANES))
    outer = np.arange(1, 9)[:, None] * np.arange(R)[None, :]
    angle = 2 * np.pi / D * outer.reshape(-1, 1) * ones
    cos_c, sin_c = np.cos(angle), np.sin(angle)
    lane_i = (np.arange(LANES) % I)[None, :]
    angle = 2 * np.pi / N * (np.arange(R)[:, None] * lane_i)
    cos_r, sin_r = np.cos(angle), np.sin(angle)
    angle = 2 * np.pi / 128 * (np.arange(C)[:, None] * lane_i % 128)
    cos_k, sin_k = np.cos(angle), np.sin(angle)
    angle = 2 * np.pi / I * (np.arange(I)[:, None] * np.arange(I)[None, :] % I)
    c, s = np.cos(angle), np.sin(angle)
    forward = np.zeros((2, LANES, 2, 2, LANES))
    backward = np.zeros((2, 2, LANES, 2, LANES))
    for slot in range(5):
        for field in range(2):
            here = slice(16 * slot + I * field, 16 * slot + I * field + I)
            for g in range(2):
                there = slice(64 * g + 16 * (slot % 4) + I * field, 64 * g + 16 * (slot % 4) + I * field + I)
                turn_i = ((c, -s), (s, c)) if slot < 4 else ((-s, -c), (c, -s))
                for part in range(2):
                    backward[g, 0, here, part, there] += turn_i[part][0]
                    backward[g, 1, here, part, there] += turn_i[part][1]
            for kind, taken in enumerate((field, 2)):
                start = 32 * slot + I * taken if slot < 4 else 32 * taken + 3 * I
                there = slice(start, start + I)
                forward[0, there, kind, 0, here], forward[1, there, kind, 0, here] = c, s
                forward[0, there, kind, 1, here], forward[1, there, kind, 1, here] = -s, c
    forward = forward.reshape(2 * LANES, 4 * LANES)
    backward = backward.reshape(4 * LANES, 2 * LANES)
    lane = np.arange(LANES)[None, :]
    row = np.arange(D)[:, None]
    p = 8 * (row // LANES) + row % 8 + R * (row % LANES // 8) + D * (lane % I)
    angular = 2 * np.pi * np.where(2 * p < N, p, p - N)
    decay = -np.where(lane // I % 2 == 0, SUBSTRATE_DIFFUSION, ACTIVATOR_DIFFUSION) * angular**2

    def parts(matrix):
        high = matrix.astype(np.float32).astype(jnp.bfloat16)
        return high, (matrix - high.astype(np.float64)).astype(jnp.bfloat16)

    along_y = [a.astype(f32) for a in (cos_y, sin_y)]
    along_x = [a.astype(f32) for a in (cos_c, sin_c, cos_r, sin_r, cos_k, sin_k, decay)]
    return (
        (*along_y, *parts(y_matrix)),
        (*along_x, *parts(forward), *parts(backward)),
        (*along_y, *parts(y_inverse)),
    )


def column_factors(place):
    lane = lane_of((1, LANES))
    slot = lane >> 4
    q = jnp.where(slot == 4, N // 2, place[1] + C * (R * (slot & 3) + place[0]))
    signed = jnp.where(2 * q < N, q, q - N).astype(jnp.float32)
    angular = 2.0 * math.pi * signed
    substrate = (lane & I) == 0
    diffusion = jnp.where(substrate, SUBSTRATE_DIFFUSION, ACTIVATOR_DIFFUSION)
    decay = jnp.where(substrate, FEED_RATE, FEED_RATE + KILL_RATE)
    normalize = 1.0 / (N * N)
    return -diffusion * (angular * angular) - decay, jnp.where(substrate, -normalize, normalize)


def call(body, out_shape, scratch, *operands, scalars=0):
    spaces = [pl.BlockSpec(memory_space=pltpu.SMEM if k < scalars else pltpu.VMEM) for k in range(len(operands))]
    return pl.pallas_call(
        body,
        out_shape=jax.ShapeDtypeStruct(out_shape, jnp.float32),
        in_specs=spaces,
        out_specs=pl.BlockSpec(memory_space=pltpu.VMEM),
        scratch_shapes=[pltpu.VMEM(shape[:2], *shape[2:] or (jnp.float32,)) for shape in scratch],
        compiler_params=pltpu.CompilerParams(vmem_limit_bytes=48 * 1024 * 1024),
    )(*operands)


def on_device(substrate, activator):
    along_y, along_x, back_y = tables()
    place = jnp.stack([lax.axis_index(ROW), lax.axis_index("col")])
    fields = jnp.concatenate([substrate.reshape(C, I, M), activator.reshape(C, I, M)], axis=1)
    fields, place = lax.optimization_barrier((fields, place))
    fields = lax.all_to_all(fields, "col", 0, 0, tiled=True)
    pieces = call(y_forward, (2 * D, LANES), [(D, 2 * M)], fields, *along_y)
    lines = lax.all_to_all(pieces.reshape(D, 2, LANES), ALL, 0, 0, tiled=True).reshape(2 * D, LANES)
    scratch = [(24 * R, LANES)] * 2 + [(D, LANES)] * 2 + [(D, 2 * LANES)]
    scratch += [(2 * LANES, 4 * LANES, jnp.bfloat16)] * 2 + [(7 * R, LANES)] * 2
    pieces = call(x_section, (D, LANES), scratch, place, lines, *along_x, scalars=1)
    pieces = lax.all_to_all(pieces.reshape(D, 1, LANES), ALL, 0, 0, tiled=True).reshape(D, LANES)
    fields = call(y_backward, (C, 2 * I, M), [(M, M), (M, 2 * M)], pieces, *back_y)
    fields = lax.all_to_all(fields, "col", 0, 0, tiled=True)
    return (fields[:, :I].reshape(C * I, M), fields[:, I:].reshape(C * I, M))


def solution(mesh):
    split = Mesh(
        mesh.devices.reshape(8, 2, 2, mesh.shape["col"]), ("row_0", "row_1", "row_2", "col")
    )
    placed = (P(ROW, "col"), P(ROW, "col"))
    return jax.shard_map(on_device, mesh=split, in_specs=placed, out_specs=placed, check_vma=False)
```

```python
import math

import jax
import jax.numpy as jnp
import numpy as np
from jax import lax
from jax.experimental import pallas as pl
from jax.experimental.pallas import tpu as pltpu
from jax.sharding import Mesh
from jax.sharding import PartitionSpec as P

ROW = ("row_0", "row_1", "row_2")
ROW_BY_CORE = ("row_2", "row_0", "row_1")
ALL = (*ROW_BY_CORE, "col")

FEED_RATE = 0.037
KILL_RATE = 0.06
TIME_STEP = 8.0
SUBSTRATE_DIFFUSION = 4e-07
ACTIVATOR_DIFFUSION = 2e-07

N = 4096
R = 32
C = 16
I = 8
M = 256
D = R * C
LANES = 128


def add(a, b):
    return b if a is None else a if b is None else a + b


def sub(a, b):
    return (None if b is None else -b) if a is None else a if b is None else a - b


def scale(a, c):
    if a is None or c == 0.0:
        return None
    return a if c == 1.0 else -a if c == -1.0 else a * c


def turn(z, k, n, sign):
    c, s = unit(k, n, sign)
    return sub(scale(z[0], c), scale(z[1], s)), add(scale(z[0], s), scale(z[1], c))


def unit(k, n, sign):
    quarter, rest = divmod(4 * (k % n), n)
    if rest == 0:
        c, s = ((1.0, 0.0), (0.0, 1.0), (-1.0, 0.0), (0.0, -1.0))[quarter]
    else:
        c, s = math.cos(2 * math.pi * k / n), math.sin(2 * math.pi * k / n)
    return c, sign * s


def dft(values, sign):
    n = len(values)
    if n == 1:
        return values
    even, odd = dft(values[0::2], sign), dft(values[1::2], sign)
    odd = [turn(z, k, n, sign) for k, z in enumerate(odd)]
    pairs = list(zip(even, odd))
    return [(add(e[0], o[0]), add(e[1], o[1])) for e, o in pairs] + [
        (sub(e[0], o[0]), sub(e[1], o[1])) for e, o in pairs
    ]


def real_dft(values):
    n = len(values)
    if n == 2:
        return [(add(*values), None), (sub(*values), None)]
    even, odd = real_dft(values[0::2]), real_dft(values[1::2])
    odd = [turn(z, k, n, -1) for k, z in enumerate(odd)]
    low = [(add(e[0], o[0]), add(e[1], o[1])) for e, o in zip(even, odd)]
    high = [(sub(e[0], o[0]), sub(o[1], e[1])) for e, o in zip(even, odd)]
    return low + high[: n // 4][::-1]


def halves(a):
    high = a.astype(jnp.bfloat16)
    return high, (a - high.astype(jnp.float32)).astype(jnp.bfloat16)


def dot(a, b, dims=((1,), (0,))):
    def product(u, v):
        return lax.dot_general(u, v, (dims, ((), ())), preferred_element_type=jnp.float32)

    return product(a[0], b[0]) + (product(a[1], b[0]) + product(a[0], b[1]))


def lane_of(shape):
    return lax.broadcasted_iota(jnp.int32, shape, len(shape) - 1)


def by_block(sources, width, lane):
    piece = sources[0]
    for k, source in enumerate(sources[1:], 1):
        piece = jnp.where(lane >= width * k, source, piece)
    return piece


def y_forward(fields, cos_y, sin_y, high, low, out, turned):
    for f in range(3):
        lines = []
        for c in range(C):
            if f < 2:
                lines.append(fields[c, f * I : (f + 1) * I, :])
            else:
                a = fields[c, I:, :]
                lines.append(fields[c, :I, :] * a * a)
        half = real_dft(lines)
        for k in range(C):
            re, im = half[k] if k <= C // 2 else half[C - k]
            if im is not None and k > C // 2:
                im = -im
            if k:
                c, s = cos_y[k : k + 1, :], sin_y[k : k + 1, :]
                if im is None:
                    re, im = re * c, -re * s
                else:
                    re, im = re * c + im * s, im * c - re * s
            else:
                im = jnp.zeros_like(re)
            row = k * 32 + f * I
            turned[row : row + I, :M] = re
            turned[row : row + I, M:] = im
    for k in range(C):
        row = k * 32 + 3 * I
        turned[row : row + I, :] = jnp.zeros((I, 2 * M), jnp.float32)
    parity = 1.0 - 2.0 * (lane_of((I, M)) & 1).astype(jnp.float32)
    place = lane_of((I, LANES))
    last = jnp.zeros((I, LANES), jnp.float32)
    for f in range(3):
        total = jnp.sum(turned[f * I : (f + 1) * I, :M] * parity, axis=1, keepdims=True)
        last = jnp.where(place == 32 * f, total, last)
    lane = lane_of((R, LANES))
    for t in range(4):
        spectra = dot(halves(turned[t * LANES : (t + 1) * LANES, :]), (high[...], low[...]))
        for part in range(2):
            half = spectra[:, part * LANES : (part + 1) * LANES]
            if t == 0 and part == 0:
                half = jnp.concatenate([half[: 3 * I], last, half[4 * I :]], axis=0)
            half = half.T
            blocks = [half[32 * s : 32 * (s + 1), :] for s in range(4)]
            blocks = [blocks[0]] + [pltpu.roll(blocks[s], 32 * s, 1) for s in range(1, 4)]
            for j in range(4):
                piece = by_block([blocks[(k - j) % 4] for k in range(4)], 32, lane)
                out[pl.ds((4 * t + j) * 2 + part, R, stride=2 * C), :] = piece


def sent(r):
    return r % 2 * (R // 2) + r // 2


def x_section(
    place, lines, cos_c, sin_c, cos_r, sin_r, cos_k, sin_k, decay, fh, fl, bh, bl, out, a_re, a_im, cos_i, sin_i, wide, gh, gl, late_c, late_s
):
    for part in range(2):
        for slot in range(4):
            here = slice(LANES * part + 32 * slot, LANES * part + 32 * (slot + 1))
            there = pl.ds(pl.multiple_of(LANES * part + 32 * ((slot + place[1]) & 3), 32), 32)
            gh[there, :] = fh[here, :]
            gl[there, :] = fl[here, :]
    for h in range(2):
        values = [
            tuple(lines[pl.ds(32 * sent(r) + 16 * h + part, 8, stride=2), :] for part in range(2))
            for r in range(R)
        ]
        for k, (re, im) in enumerate(dft(values, -1)):
            a_re[k * 24 + 8 * h : k * 24 + 8 * h + 8, :] = re
            a_im[k * 24 + 8 * h : k * 24 + 8 * h + 8, :] = im

    def turn_c(c, h):
        rows = slice((c - 1) * R + 8 * h, (c - 1) * R + 8 * h + 8)
        if c <= 8:
            return cos_c[rows, :], sin_c[rows, :]
        rows = slice((c - 9) * R + 8 * h, (c - 9) * R + 8 * h + 8)
        return late_c[rows, :], late_s[rows, :]

    for h in range(4):
        values = []
        for c in range(C):
            re, im = a_re[pl.ds(8 * h * 24 + c, 8, stride=24), :], a_im[pl.ds(8 * h * 24 + c, 8, stride=24), :]
            if c > 8:
                (u, v), (w, z) = turn_c(c - 8, h), turn_c(8, h)
                rows = slice((c - 9) * R + 8 * h, (c - 9) * R + 8 * h + 8)
                late_c[rows, :], late_s[rows, :] = u * w - v * z, u * z + v * w
            if c:
                u, v = turn_c(c, h)
                re, im = re * u + im * v, im * u - re * v
            values.append((re, im))
        for k, (re, im) in enumerate(dft(values, -1)):
            rows = slice(h * LANES + 8 * k, h * LANES + 8 * k + 8)
            u, v = cos_r[8 * h : 8 * h + 8, :], sin_r[8 * h : 8 * h + 8, :]
            if k:
                c, d = cos_k[k : k + 1, :], sin_k[k : k + 1, :]
                u, v = u * c - v * d, u * d + v * c
            cos_i[rows, :], sin_i[rows, :] = u, v
            wide[rows, :LANES] = re * u + im * v
            wide[rows, LANES:] = im * u - re * v
    along_y, normal = column_factors(place)
    low_lanes = lane_of((8, LANES)) < 64
    for g in range(2):
        advanced = []
        for h in (2 * g, 2 * g + 1):
            rows = slice(h * LANES, (h + 1) * LANES)
            spectra = dot(halves(wide[rows, :]), (gh[...], gl[...]))
            linear = decay[rows, :] + along_y
            grown = jnp.exp(linear * (0.5 * TIME_STEP))
            growth, forcing = grown * (1.0 / (N * N)), (grown - 1.0) / linear * normal
            advanced.append(growth * spectra[:, :LANES] + forcing * spectra[:, 2 * LANES : 3 * LANES])
            advanced.append(growth * spectra[:, LANES : 2 * LANES] + forcing * spectra[:, 3 * LANES :])
        both = dot(halves(jnp.concatenate(advanced, axis=1)), (bh[...], bl[...]))
        values = []
        for k in range(C):
            rows = [slice(h * LANES + 8 * k, h * LANES + 8 * k + 8) for h in (2 * g, 2 * g + 1)]
            u, v = (jnp.where(low_lanes, t[rows[0], :], t[rows[1], :]) for t in (cos_i, sin_i))
            re, im = both[8 * k : 8 * k + 8, :LANES], both[8 * k : 8 * k + 8, LANES:]
            values.append((re * u - im * v, im * u + re * v))
        values = dft(values, 1)
        for c in range(1, C):
            first, second = turn_c(c, 2 * g), turn_c(c, 2 * g + 1)
            u, v = jnp.where(low_lanes, first[0], second[0]), jnp.where(low_lanes, first[1], second[1])
            re, im = values[c]
            values[c] = re * u - im * v, im * u + re * v
        for c in range(8):
            for part, kept in enumerate((a_re, a_im)):
                one, two = values[c][part], values[c + 8][part]
                kept[pl.ds(128 * g + c, 8, stride=8), :] = jnp.where(low_lanes, one, pltpu.roll(two, 64, 1))
                kept[pl.ds(128 * g + 64 + c, 8, stride=8), :] = jnp.where(low_lanes, pltpu.roll(one, 64, 1), two)
    on = 16 * (place[1] & 7)
    values = [(a_re[8 * k : 8 * k + 8, :], a_im[8 * k : 8 * k + 8, :]) for k in range(R)]
    for r, (re, im) in enumerate(dft(values, 1)):
        one = jnp.where(low_lanes, re, pltpu.roll(im, 64, 1))
        two = jnp.where(low_lanes, pltpu.roll(re, 64, 1), im)
        row = C * sent(r)
        out[row : row + 8, :] = pltpu.roll(one, on, 1)
        out[row + 8 : row + 16, :] = pltpu.roll(two, on, 1)


def y_backward(pieces, cos_y, sin_y, high, low, out, spectrum, turned):
    lane = lane_of((R, LANES))
    for t in range(2):
        sources = [pieces[pl.ds(8 * t + j, R, stride=C), :] for j in range(8)]
        for b in range(8):
            block = by_block([sources[(k - b) % 8] for k in range(8)], 16, lane)
            block = pltpu.roll(block, LANES - 16 * b, 1) if b else block
            spectrum[b * R : (b + 1) * R, t * LANES : (t + 1) * LANES] = block
    flipped = spectrum[...].T
    turned[...] = dot(halves(flipped), (high[...], low[...]))
    parity = 1.0 - 2.0 * (lane_of((16, M)) & 1).astype(jnp.float32)
    values = []
    for k in range(C):
        re, im = turned[16 * k : 16 * (k + 1), :M], turned[16 * k : 16 * (k + 1), M:]
        if k == 0:
            re, im = re - flipped[:16, 0:1] + flipped[:16, 128:129] * parity, None
        else:
            u, v = cos_y[k : k + 1, :], sin_y[k : k + 1, :]
            re, im = re * u - im * v, im * u + re * v
        values.append((re, im))
    substrate_row = lax.broadcasted_iota(jnp.int32, (16, M), 0) < I
    constant = math.expm1(-0.5 * FEED_RATE * TIME_STEP) / -FEED_RATE * FEED_RATE
    shift = jnp.where(substrate_row, constant, 0.0)
    for c, (re, _) in enumerate(dft(values, 1)):
        out[c] = re + shift


def tables():
    f32 = np.float32
    angle = 2 * np.pi / N * (np.arange(C)[:, None] * np.arange(M)[None, :])
    cos_y, sin_y = np.cos(angle), np.sin(angle)
    turn_m = 2 * np.pi / M * (np.arange(M)[:, None] * np.arange(128)[None, :] % M)
    c, s = np.cos(turn_m), np.sin(turn_m)
    y_matrix = np.block([[c, -s], [s, c]])
    y_inverse = 2 * np.block([[c.T, s.T], [-s.T, c.T]])
    ones = np.ones((1, LANES))
    outer = np.arange(1, 9)[:, None] * np.arange(R)[None, :]
    angle = 2 * np.pi / D * outer.reshape(-1, 1) * ones
    cos_c, sin_c = np.cos(angle), np.sin(angle)
    lane_i = (np.arange(LANES) % I)[None, :]
    angle = 2 * np.pi / N * (np.arange(R)[:, None] * lane_i)
    cos_r, sin_r = np.cos(angle), np.sin(angle)
    angle = 2 * np.pi / 128 * (np.arange(C)[:, None] * lane_i % 128)
    cos_k, sin_k = np.cos(angle), np.sin(angle)
    angle = 2 * np.pi / I * (np.arange(I)[:, None] * np.arange(I)[None, :] % I)
    c, s = np.cos(angle), np.sin(angle)
    forward = np.zeros((2, LANES, 2, 2, LANES))
    backward = np.zeros((2, 2, LANES, 2, LANES))
    for slot in range(5):
        for field in range(2):
            here = slice(16 * slot + I * field, 16 * slot + I * field + I)
            for g in range(2):
                there = slice(64 * g + 16 * (slot % 4) + I * field, 64 * g + 16 * (slot % 4) + I * field + I)
                turn_i = ((c, -s), (s, c)) if slot < 4 else ((-s, -c), (c, -s))
                for part in range(2):
                    backward[g, 0, here, part, there] += turn_i[part][0]
                    backward[g, 1, here, part, there] += turn_i[part][1]
            for kind, taken in enumerate((field, 2)):
                start = 32 * slot + I * taken if slot < 4 else 32 * taken + 3 * I
                there = slice(start, start + I)
                forward[0, there, kind, 0, here], forward[1, there, kind, 0, here] = c, s
                forward[0, there, kind, 1, here], forward[1, there, kind, 1, here] = -s, c
    forward = forward.reshape(2 * LANES, 4 * LANES)
    backward = backward.reshape(4 * LANES, 2 * LANES)
    lane = np.arange(LANES)[None, :]
    row = np.arange(D)[:, None]
    p = 8 * (row // LANES) + row % 8 + R * (row % LANES // 8) + D * (lane % I)
    angular = 2 * np.pi * np.where(2 * p < N, p, p - N)
    decay = -np.where(lane // I % 2 == 0, SUBSTRATE_DIFFUSION, ACTIVATOR_DIFFUSION) * angular**2

    def parts(matrix):
        high = matrix.astype(np.float32).astype(jnp.bfloat16)
        return high, (matrix - high.astype(np.float64)).astype(jnp.bfloat16)

    along_y = [a.astype(f32) for a in (cos_y, sin_y)]
    along_x = [a.astype(f32) for a in (cos_c, sin_c, cos_r, sin_r, cos_k, sin_k, decay)]
    return (
        (*along_y, *parts(y_matrix)),
        (*along_x, *parts(forward), *parts(backward)),
        (*along_y, *parts(y_inverse)),
    )


def column_factors(place):
    lane = lane_of((1, LANES))
    slot = lane >> 4
    q = jnp.where(slot == 4, N // 2, place[1] + C * (R * (slot & 3) + place[0]))
    signed = jnp.where(2 * q < N, q, q - N).astype(jnp.float32)
    angular = 2.0 * math.pi * signed
    substrate = (lane & I) == 0
    diffusion = jnp.where(substrate, SUBSTRATE_DIFFUSION, ACTIVATOR_DIFFUSION)
    decay = jnp.where(substrate, FEED_RATE, FEED_RATE + KILL_RATE)
    normalize = 1.0 / (N * N)
    return -diffusion * (angular * angular) - decay, jnp.where(substrate, -normalize, normalize)


def call(body, out_shape, scratch, *operands, scalars=0):
    spaces = [pl.BlockSpec(memory_space=pltpu.SMEM if k < scalars else pltpu.VMEM) for k in range(len(operands))]
    return pl.pallas_call(
        body,
        out_shape=jax.ShapeDtypeStruct(out_shape, jnp.float32),
        in_specs=spaces,
        out_specs=pl.BlockSpec(memory_space=pltpu.VMEM),
        scratch_shapes=[pltpu.VMEM(shape[:2], *shape[2:] or (jnp.float32,)) for shape in scratch],
        compiler_params=pltpu.CompilerParams(vmem_limit_bytes=48 * 1024 * 1024),
    )(*operands)


def on_device(substrate, activator):
    along_y, along_x, back_y = tables()
    place = jnp.stack([lax.axis_index(ROW_BY_CORE), lax.axis_index("col")])
    fields = jnp.concatenate([substrate.reshape(C, I, M), activator.reshape(C, I, M)], axis=1)
    fields, place = lax.optimization_barrier((fields, place))
    fields = lax.all_to_all(fields, "col", 0, 0, tiled=True)
    pieces = call(y_forward, (2 * D, LANES), [(D, 2 * M)], fields, *along_y)
    lines = lax.all_to_all(pieces.reshape(D, 2, LANES), ALL, 0, 0, tiled=True).reshape(2 * D, LANES)
    scratch = [(24 * R, LANES)] * 2 + [(D, LANES)] * 2 + [(D, 2 * LANES)]
    scratch += [(2 * LANES, 4 * LANES, jnp.bfloat16)] * 2 + [(7 * R, LANES)] * 2
    pieces = call(x_section, (D, LANES), scratch, place, lines, *along_x, scalars=1)
    pieces = lax.all_to_all(pieces.reshape(D, 1, LANES), ALL, 0, 0, tiled=True).reshape(D, LANES)
    fields = call(y_backward, (C, 2 * I, M), [(M, M), (M, 2 * M)], pieces, *back_y)
    fields = lax.all_to_all(fields, "col", 0, 0, tiled=True)
    return (fields[:, :I].reshape(C * I, M), fields[:, I:].reshape(C * I, M))


def solution(mesh):
    split = Mesh(
        mesh.devices.reshape(8, 2, 2, mesh.shape["col"]), ("row_0", "row_1", "row_2", "col")
    )
    placed = (P(ROW, "col"), P(ROW, "col"))
    return jax.shard_map(on_device, mesh=split, in_specs=placed, out_specs=placed, check_vma=False)
```

```python
import math

import jax
import jax.numpy as jnp
import numpy as np
from jax import lax
from jax.experimental import pallas as pl
from jax.experimental.pallas import tpu as pltpu
from jax.sharding import Mesh
from jax.sharding import PartitionSpec as P

ROW = ("row_0", "row_1", "row_2")
ALL = ("row_0", "row_1", "row_2", "col")

FEED_RATE = 0.037
KILL_RATE = 0.06
TIME_STEP = 8.0
SUBSTRATE_DIFFUSION = 4e-07
ACTIVATOR_DIFFUSION = 2e-07

N = 4096
R = 32
C = 16
I = 8
M = 256
D = R * C
LANES = 128


def add(a, b):
    return b if a is None else a if b is None else a + b


def sub(a, b):
    return (None if b is None else -b) if a is None else a if b is None else a - b


def scale(a, c):
    if a is None or c == 0.0:
        return None
    return a if c == 1.0 else -a if c == -1.0 else a * c


def turn(z, k, n, sign):
    c, s = unit(k, n, sign)
    return sub(scale(z[0], c), scale(z[1], s)), add(scale(z[0], s), scale(z[1], c))


def unit(k, n, sign):
    quarter, rest = divmod(4 * (k % n), n)
    if rest == 0:
        c, s = ((1.0, 0.0), (0.0, 1.0), (-1.0, 0.0), (0.0, -1.0))[quarter]
    else:
        c, s = math.cos(2 * math.pi * k / n), math.sin(2 * math.pi * k / n)
    return c, sign * s


def dft(values, sign):
    n = len(values)
    if n == 1:
        return values
    even, odd = dft(values[0::2], sign), dft(values[1::2], sign)
    odd = [turn(z, k, n, sign) for k, z in enumerate(odd)]
    pairs = list(zip(even, odd))
    return [(add(e[0], o[0]), add(e[1], o[1])) for e, o in pairs] + [
        (sub(e[0], o[0]), sub(e[1], o[1])) for e, o in pairs
    ]


def real_dft(values):
    n = len(values)
    if n == 2:
        return [(add(*values), None), (sub(*values), None)]
    even, odd = real_dft(values[0::2]), real_dft(values[1::2])
    odd = [turn(z, k, n, -1) for k, z in enumerate(odd)]
    low = [(add(e[0], o[0]), add(e[1], o[1])) for e, o in zip(even, odd)]
    high = [(sub(e[0], o[0]), sub(o[1], e[1])) for e, o in zip(even, odd)]
    return low + high[: n // 4][::-1]


def halves(a):
    high = a.astype(jnp.bfloat16)
    return high, (a - high.astype(jnp.float32)).astype(jnp.bfloat16)


def dot(a, b, dims=((1,), (0,))):
    def product(u, v):
        return lax.dot_general(u, v, (dims, ((), ())), preferred_element_type=jnp.float32)

    return product(a[0], b[0]) + (product(a[1], b[0]) + product(a[0], b[1]))


def lane_of(shape):
    return lax.broadcasted_iota(jnp.int32, shape, len(shape) - 1)


def by_block(sources, width, lane):
    piece = sources[0]
    for k, source in enumerate(sources[1:], 1):
        piece = jnp.where(lane >= width * k, source, piece)
    return piece


def y_forward(fields, cos_y, sin_y, high, low, out, turned):
    for f in range(3):
        lines = []
        for c in range(C):
            if f < 2:
                lines.append(fields[c, f * I : (f + 1) * I, :])
            else:
                a = fields[c, I:, :]
                lines.append(fields[c, :I, :] * a * a)
        half = real_dft(lines)
        for k in range(C):
            re, im = half[k] if k <= C // 2 else half[C - k]
            if im is not None and k > C // 2:
                im = -im
            if k:
                c, s = cos_y[k : k + 1, :], sin_y[k : k + 1, :]
                if im is None:
                    re, im = re * c, -re * s
                else:
                    re, im = re * c + im * s, im * c - re * s
            else:
                im = jnp.zeros_like(re)
            row = k * 32 + f * I
            turned[row : row + I, :M] = re
            turned[row : row + I, M:] = im
    for k in range(C):
        row = k * 32 + 3 * I
        turned[row : row + I, :] = jnp.zeros((I, 2 * M), jnp.float32)
    parity = 1.0 - 2.0 * (lane_of((I, M)) & 1).astype(jnp.float32)
    place = lane_of((I, LANES))
    last = jnp.zeros((I, LANES), jnp.float32)
    for f in range(3):
        total = jnp.sum(turned[f * I : (f + 1) * I, :M] * parity, axis=1, keepdims=True)
        last = jnp.where(place == 32 * f, total, last)
    lane = lane_of((R, LANES))
    for t in range(4):
        spectra = dot(halves(turned[t * LANES : (t + 1) * LANES, :]), (high[...], low[...]))
        for part in range(2):
            half = spectra[:, part * LANES : (part + 1) * LANES]
            if t == 0 and part == 0:
                half = jnp.concatenate([half[: 3 * I], last, half[4 * I :]], axis=0)
            half = half.T
            blocks = [half[32 * s : 32 * (s + 1), :] for s in range(4)]
            blocks = [blocks[0]] + [pltpu.roll(blocks[s], 32 * s, 1) for s in range(1, 4)]
            for j in range(4):
                piece = by_block([blocks[(k - j) % 4] for k in range(4)], 32, lane)
                out[pl.ds((4 * t + j) * 2 + part, R, stride=2 * C), :] = piece


def x_section(
    lines, cos_c, sin_c, cos_r, sin_r, cos_k, sin_k, decay, fh, fl, bh, bl, out, a_re, a_im, cos_i, sin_i, wide, gh, gl, late_c, late_s
):
    place = lax.axis_index(ROW), lax.axis_index("col")
    for part in range(2):
        for slot in range(4):
            here = slice(LANES * part + 32 * slot, LANES * part + 32 * (slot + 1))
            there = pl.ds(pl.multiple_of(LANES * part + 32 * ((slot + place[1]) & 3), 32), 32)
            gh[there, :] = fh[here, :]
            gl[there, :] = fl[here, :]
    for h in range(2):
        values = [
            tuple(lines[pl.ds(32 * r + 16 * h + part, 8, stride=2), :] for part in range(2)) for r in range(R)
        ]
        for k, (re, im) in enumerate(dft(values, -1)):
            a_re[k * 24 + 8 * h : k * 24 + 8 * h + 8, :] = re
            a_im[k * 24 + 8 * h : k * 24 + 8 * h + 8, :] = im

    def turn_c(c, h):
        rows = slice((c - 1) * R + 8 * h, (c - 1) * R + 8 * h + 8)
        if c <= 8:
            return cos_c[rows, :], sin_c[rows, :]
        rows = slice((c - 9) * R + 8 * h, (c - 9) * R + 8 * h + 8)
        return late_c[rows, :], late_s[rows, :]

    for h in range(4):
        values = []
        for c in range(C):
            re, im = a_re[pl.ds(8 * h * 24 + c, 8, stride=24), :], a_im[pl.ds(8 * h * 24 + c, 8, stride=24), :]
            if c > 8:
                (u, v), (w, z) = turn_c(c - 8, h), turn_c(8, h)
                rows = slice((c - 9) * R + 8 * h, (c - 9) * R + 8 * h + 8)
                late_c[rows, :], late_s[rows, :] = u * w - v * z, u * z + v * w
            if c:
                u, v = turn_c(c, h)
                re, im = re * u + im * v, im * u - re * v
            values.append((re, im))
        for k, (re, im) in enumerate(dft(values, -1)):
            rows = slice(h * LANES + 8 * k, h * LANES + 8 * k + 8)
            u, v = cos_r[8 * h : 8 * h + 8, :], sin_r[8 * h : 8 * h + 8, :]
            if k:
                c, d = cos_k[k : k + 1, :], sin_k[k : k + 1, :]
                u, v = u * c - v * d, u * d + v * c
            cos_i[rows, :], sin_i[rows, :] = u, v
            wide[rows, :LANES] = re * u + im * v
            wide[rows, LANES:] = im * u - re * v
    along_y, normal = column_factors(place)
    low_lanes = lane_of((8, LANES)) < 64
    for g in range(2):
        advanced = []
        for h in (2 * g, 2 * g + 1):
            rows = slice(h * LANES, (h + 1) * LANES)
            spectra = dot(halves(wide[rows, :]), (gh[...], gl[...]))
            linear = decay[rows, :] + along_y
            grown = jnp.exp(linear * (0.5 * TIME_STEP))
            growth, forcing = grown * (1.0 / (N * N)), (grown - 1.0) / linear * normal
            advanced.append(growth * spectra[:, :LANES] + forcing * spectra[:, 2 * LANES : 3 * LANES])
            advanced.append(growth * spectra[:, LANES : 2 * LANES] + forcing * spectra[:, 3 * LANES :])
        both = dot(halves(jnp.concatenate(advanced, axis=1)), (bh[...], bl[...]))
        values = []
        for k in range(C):
            rows = [slice(h * LANES + 8 * k, h * LANES + 8 * k + 8) for h in (2 * g, 2 * g + 1)]
            u, v = (jnp.where(low_lanes, t[rows[0], :], t[rows[1], :]) for t in (cos_i, sin_i))
            re, im = both[8 * k : 8 * k + 8, :LANES], both[8 * k : 8 * k + 8, LANES:]
            values.append((re * u - im * v, im * u + re * v))
        values = dft(values, 1)
        for c in range(1, C):
            first, second = turn_c(c, 2 * g), turn_c(c, 2 * g + 1)
            u, v = jnp.where(low_lanes, first[0], second[0]), jnp.where(low_lanes, first[1], second[1])
            re, im = values[c]
            values[c] = re * u - im * v, im * u + re * v
        for c in range(8):
            for part, kept in enumerate((a_re, a_im)):
                one, two = values[c][part], values[c + 8][part]
                kept[pl.ds(128 * g + c, 8, stride=8), :] = jnp.where(low_lanes, one, pltpu.roll(two, 64, 1))
                kept[pl.ds(128 * g + 64 + c, 8, stride=8), :] = jnp.where(low_lanes, pltpu.roll(one, 64, 1), two)
    on = 16 * (place[1] & 7)
    values = [(a_re[8 * k : 8 * k + 8, :], a_im[8 * k : 8 * k + 8, :]) for k in range(R)]
    for r, (re, im) in enumerate(dft(values, 1)):
        one = jnp.where(low_lanes, re, pltpu.roll(im, 64, 1))
        two = jnp.where(low_lanes, pltpu.roll(re, 64, 1), im)
        out[r * C : r * C + 8, :] = pltpu.roll(one, on, 1)
        out[r * C + 8 : r * C + 16, :] = pltpu.roll(two, on, 1)


def y_backward(pieces, cos_y, sin_y, high, low, out, spectrum, turned):
    lane = lane_of((R, LANES))
    for t in range(2):
        sources = [pieces[pl.ds(8 * t + j, R, stride=C), :] for j in range(8)]
        for b in range(8):
            block = by_block([sources[(k - b) % 8] for k in range(8)], 16, lane)
            block = pltpu.roll(block, LANES - 16 * b, 1) if b else block
            spectrum[b * R : (b + 1) * R, t * LANES : (t + 1) * LANES] = block
    flipped = spectrum[...].T
    turned[...] = dot(halves(flipped), (high[...], low[...]))
    parity = 1.0 - 2.0 * (lane_of((16, M)) & 1).astype(jnp.float32)
    values = []
    for k in range(C):
        re, im = turned[16 * k : 16 * (k + 1), :M], turned[16 * k : 16 * (k + 1), M:]
        if k == 0:
            re, im = re - flipped[:16, 0:1] + flipped[:16, 128:129] * parity, None
        else:
            u, v = cos_y[k : k + 1, :], sin_y[k : k + 1, :]
            re, im = re * u - im * v, im * u + re * v
        values.append((re, im))
    substrate_row = lax.broadcasted_iota(jnp.int32, (16, M), 0) < I
    constant = math.expm1(-0.5 * FEED_RATE * TIME_STEP) / -FEED_RATE * FEED_RATE
    shift = jnp.where(substrate_row, constant, 0.0)
    for c, (re, _) in enumerate(dft(values, 1)):
        out[c] = re + shift


def tables():
    f32 = np.float32
    angle = 2 * np.pi / N * (np.arange(C)[:, None] * np.arange(M)[None, :])
    cos_y, sin_y = np.cos(angle), np.sin(angle)
    turn_m = 2 * np.pi / M * (np.arange(M)[:, None] * np.arange(128)[None, :] % M)
    c, s = np.cos(turn_m), np.sin(turn_m)
    y_matrix = np.block([[c, -s], [s, c]])
    y_inverse = 2 * np.block([[c.T, s.T], [-s.T, c.T]])
    ones = np.ones((1, LANES))
    outer = np.arange(1, 9)[:, None] * np.arange(R)[None, :]
    angle = 2 * np.pi / D * outer.reshape(-1, 1) * ones
    cos_c, sin_c = np.cos(angle), np.sin(angle)
    lane_i = (np.arange(LANES) % I)[None, :]
    angle = 2 * np.pi / N * (np.arange(R)[:, None] * lane_i)
    cos_r, sin_r = np.cos(angle), np.sin(angle)
    angle = 2 * np.pi / 128 * (np.arange(C)[:, None] * lane_i % 128)
    cos_k, sin_k = np.cos(angle), np.sin(angle)
    angle = 2 * np.pi / I * (np.arange(I)[:, None] * np.arange(I)[None, :] % I)
    c, s = np.cos(angle), np.sin(angle)
    forward = np.zeros((2, LANES, 2, 2, LANES))
    backward = np.zeros((2, 2, LANES, 2, LANES))
    for slot in range(5):
        for field in range(2):
            here = slice(16 * slot + I * field, 16 * slot + I * field + I)
            for g in range(2):
                there = slice(64 * g + 16 * (slot % 4) + I * field, 64 * g + 16 * (slot % 4) + I * field + I)
                turn_i = ((c, -s), (s, c)) if slot < 4 else ((-s, -c), (c, -s))
                for part in range(2):
                    backward[g, 0, here, part, there] += turn_i[part][0]
                    backward[g, 1, here, part, there] += turn_i[part][1]
            for kind, taken in enumerate((field, 2)):
                start = 32 * slot + I * taken if slot < 4 else 32 * taken + 3 * I
                there = slice(start, start + I)
                forward[0, there, kind, 0, here], forward[1, there, kind, 0, here] = c, s
                forward[0, there, kind, 1, here], forward[1, there, kind, 1, here] = -s, c
    forward = forward.reshape(2 * LANES, 4 * LANES)
    backward = backward.reshape(4 * LANES, 2 * LANES)
    lane = np.arange(LANES)[None, :]
    row = np.arange(D)[:, None]
    p = 8 * (row // LANES) + row % 8 + R * (row % LANES // 8) + D * (lane % I)
    angular = 2 * np.pi * np.where(2 * p < N, p, p - N)
    decay = -np.where(lane // I % 2 == 0, SUBSTRATE_DIFFUSION, ACTIVATOR_DIFFUSION) * angular**2

    def parts(matrix):
        high = matrix.astype(np.float32).astype(jnp.bfloat16)
        return high, (matrix - high.astype(np.float64)).astype(jnp.bfloat16)

    along_y = [a.astype(f32) for a in (cos_y, sin_y)]
    along_x = [a.astype(f32) for a in (cos_c, sin_c, cos_r, sin_r, cos_k, sin_k, decay)]
    return (
        (*along_y, *parts(y_matrix)),
        (*along_x, *parts(forward), *parts(backward)),
        (*along_y, *parts(y_inverse)),
    )


def column_factors(place):
    lane = lane_of((1, LANES))
    slot = lane >> 4
    q = jnp.where(slot == 4, N // 2, place[1] + C * (R * (slot & 3) + place[0]))
    signed = jnp.where(2 * q < N, q, q - N).astype(jnp.float32)
    angular = 2.0 * math.pi * signed
    substrate = (lane & I) == 0
    diffusion = jnp.where(substrate, SUBSTRATE_DIFFUSION, ACTIVATOR_DIFFUSION)
    decay = jnp.where(substrate, FEED_RATE, FEED_RATE + KILL_RATE)
    normalize = 1.0 / (N * N)
    return -diffusion * (angular * angular) - decay, jnp.where(substrate, -normalize, normalize)


def call(body, out_shape, scratch, *operands):
    return pl.pallas_call(
        body,
        out_shape=jax.ShapeDtypeStruct(out_shape, jnp.float32),
        in_specs=[pl.BlockSpec(memory_space=pltpu.VMEM) for _ in operands],
        out_specs=pl.BlockSpec(memory_space=pltpu.VMEM),
        scratch_shapes=[pltpu.VMEM(shape[:2], *shape[2:] or (jnp.float32,)) for shape in scratch],
        compiler_params=pltpu.CompilerParams(vmem_limit_bytes=48 * 1024 * 1024),
    )(*operands)


def stack_fields(substrate, activator, out, first, second):
    copies = (
        pltpu.make_async_copy(substrate, out.at[:, :I, :], first),
        pltpu.make_async_copy(activator, out.at[:, I:, :], second),
    )
    for copy in copies:
        copy.start()
    for copy in copies:
        copy.wait()


def split_fields(fields, substrate, activator, first, second):
    copies = (
        pltpu.make_async_copy(fields.at[:, :I, :], substrate, first),
        pltpu.make_async_copy(fields.at[:, I:, :], activator, second),
    )
    for copy in copies:
        copy.start()
    for copy in copies:
        copy.wait()


def on_device(substrate, activator):
    along_y, along_x, back_y = tables()
    whole = pl.BlockSpec(memory_space=pltpu.VMEM)
    outside = pl.BlockSpec(memory_space=pl.ANY)
    one = jax.ShapeDtypeStruct((C, I, M), jnp.float32)
    small = pltpu.CompilerParams(vmem_limit_bytes=4 * 1024 * 1024)
    flags = [pltpu.SemaphoreType.DMA, pltpu.SemaphoreType.DMA]
    fields = pl.pallas_call(
        stack_fields,
        out_shape=jax.ShapeDtypeStruct((C, 2 * I, M), jnp.float32),
        in_specs=[outside, outside],
        out_specs=whole,
        scratch_shapes=flags,
        compiler_params=small,
    )(substrate.reshape(C, I, M), activator.reshape(C, I, M))
    fields = lax.all_to_all(fields, "col", 0, 0, tiled=True)
    pieces = call(y_forward, (2 * D, LANES), [(D, 2 * M)], fields, *along_y)
    lines = lax.all_to_all(pieces.reshape(D, 2, LANES), ALL, 0, 0, tiled=True).reshape(2 * D, LANES)
    scratch = [(24 * R, LANES)] * 2 + [(D, LANES)] * 2 + [(D, 2 * LANES)]
    scratch += [(2 * LANES, 4 * LANES, jnp.bfloat16)] * 2 + [(7 * R, LANES)] * 2
    pieces = call(x_section, (D, LANES), scratch, lines, *along_x)
    pieces = lax.all_to_all(pieces.reshape(D, 1, LANES), ALL, 0, 0, tiled=True).reshape(D, LANES)
    fields = call(y_backward, (C, 2 * I, M), [(M, M), (M, 2 * M)], pieces, *back_y)
    fields = lax.all_to_all(fields, "col", 0, 0, tiled=True)
    substrate, activator = pl.pallas_call(
        split_fields,
        out_shape=(one, one),
        in_specs=[whole],
        out_specs=(outside, outside),
        scratch_shapes=flags,
        compiler_params=small,
    )(fields)
    return substrate.reshape(C * I, M), activator.reshape(C * I, M)


def solution(mesh):
    split = Mesh(
        mesh.devices.reshape(8, 2, 2, mesh.shape["col"]), ("row_0", "row_1", "row_2", "col")
    )
    placed = (P(ROW, "col"), P(ROW, "col"))
    return jax.shard_map(on_device, mesh=split, in_specs=placed, out_specs=placed, check_vma=False)
```

```python
import math

import jax
import jax.numpy as jnp
import numpy as np
from jax import lax
from jax.experimental import pallas as pl
from jax.experimental.pallas import tpu as pltpu
from jax.sharding import Mesh
from jax.sharding import PartitionSpec as P

ROW = ("row_0", "row_1", "row_2")
ALL = ("row_0", "row_1", "row_2", "col")

FEED_RATE = 0.037
KILL_RATE = 0.06
TIME_STEP = 8.0
SUBSTRATE_DIFFUSION = 4e-07
ACTIVATOR_DIFFUSION = 2e-07

N = 4096
R = 32
C = 16
I = 8
M = 256
D = R * C
LANES = 128


def add(a, b):
    return b if a is None else a if b is None else a + b


def sub(a, b):
    return (None if b is None else -b) if a is None else a if b is None else a - b


def scale(a, c):
    if a is None or c == 0.0:
        return None
    return a if c == 1.0 else -a if c == -1.0 else a * c


def turn(z, k, n, sign):
    c, s = unit(k, n, sign)
    return sub(scale(z[0], c), scale(z[1], s)), add(scale(z[0], s), scale(z[1], c))


def unit(k, n, sign):
    quarter, rest = divmod(4 * (k % n), n)
    if rest == 0:
        c, s = ((1.0, 0.0), (0.0, 1.0), (-1.0, 0.0), (0.0, -1.0))[quarter]
    else:
        c, s = math.cos(2 * math.pi * k / n), math.sin(2 * math.pi * k / n)
    return c, sign * s


def dft(values, sign):
    n = len(values)
    if n == 1:
        return values
    even, odd = dft(values[0::2], sign), dft(values[1::2], sign)
    odd = [turn(z, k, n, sign) for k, z in enumerate(odd)]
    pairs = list(zip(even, odd))
    return [(add(e[0], o[0]), add(e[1], o[1])) for e, o in pairs] + [
        (sub(e[0], o[0]), sub(e[1], o[1])) for e, o in pairs
    ]


def real_dft(values):
    n = len(values)
    if n == 2:
        return [(add(*values), None), (sub(*values), None)]
    even, odd = real_dft(values[0::2]), real_dft(values[1::2])
    odd = [turn(z, k, n, -1) for k, z in enumerate(odd)]
    low = [(add(e[0], o[0]), add(e[1], o[1])) for e, o in zip(even, odd)]
    high = [(sub(e[0], o[0]), sub(o[1], e[1])) for e, o in zip(even, odd)]
    return low + high[: n // 4][::-1]


def halves(a):
    high = a.astype(jnp.bfloat16)
    return high, (a - high.astype(jnp.float32)).astype(jnp.bfloat16)


def dot(a, b, dims=((1,), (0,))):
    def product(u, v):
        return lax.dot_general(u, v, (dims, ((), ())), preferred_element_type=jnp.float32)

    return product(a[0], b[0]) + (product(a[1], b[0]) + product(a[0], b[1]))


def lane_of(shape):
    return lax.broadcasted_iota(jnp.int32, shape, len(shape) - 1)


def by_block(sources, width, lane):
    piece = sources[0]
    for k, source in enumerate(sources[1:], 1):
        piece = jnp.where(lane >= width * k, source, piece)
    return piece


def y_forward(fields, cos_y, sin_y, high, low, out, turned):
    for f in range(3):
        lines = []
        for c in range(C):
            if f < 2:
                lines.append(fields[c, f * I : (f + 1) * I, :])
            else:
                a = fields[c, I:, :]
                lines.append(fields[c, :I, :] * a * a)
        half = real_dft(lines)
        for k in range(C):
            re, im = half[k] if k <= C // 2 else half[C - k]
            if im is not None and k > C // 2:
                im = -im
            if k:
                c, s = cos_y[k : k + 1, :], sin_y[k : k + 1, :]
                if im is None:
                    re, im = re * c, -re * s
                else:
                    re, im = re * c + im * s, im * c - re * s
            else:
                im = jnp.zeros_like(re)
            row = k * 32 + f * I
            turned[row : row + I, :M] = re
            turned[row : row + I, M:] = im
    for k in range(C):
        row = k * 32 + 3 * I
        turned[row : row + I, :] = jnp.zeros((I, 2 * M), jnp.float32)
    parity = 1.0 - 2.0 * (lane_of((I, M)) & 1).astype(jnp.float32)
    place = lane_of((I, LANES))
    last = jnp.zeros((I, LANES), jnp.float32)
    for f in range(3):
        total = jnp.sum(turned[f * I : (f + 1) * I, :M] * parity, axis=1, keepdims=True)
        last = jnp.where(place == 32 * f, total, last)
    lane = lane_of((R, LANES))
    for t in range(4):
        spectra = dot(halves(turned[t * LANES : (t + 1) * LANES, :]), (high[...], low[...]))
        for part in range(2):
            half = spectra[:, part * LANES : (part + 1) * LANES]
            if t == 0 and part == 0:
                half = jnp.concatenate([half[: 3 * I], last, half[4 * I :]], axis=0)
            half = half.T
            blocks = [half[32 * s : 32 * (s + 1), :] for s in range(4)]
            blocks = [blocks[0]] + [pltpu.roll(blocks[s], 32 * s, 1) for s in range(1, 4)]
            for j in range(4):
                piece = by_block([blocks[(k - j) % 4] for k in range(4)], 32, lane)
                out[pl.ds((4 * t + j) * 2 + part, R, stride=2 * C), :] = piece


def x_section(
    lines, cos_c, sin_c, cos_r, sin_r, cos_k, sin_k, decay, fh, fl, bh, bl, out, a_re, a_im, cos_i, sin_i, wide, gh, gl, late_c, late_s
):
    place = lax.axis_index(ROW), lax.axis_index("col")
    for part in range(2):
        for slot in range(4):
            here = slice(LANES * part + 32 * slot, LANES * part + 32 * (slot + 1))
            there = pl.ds(pl.multiple_of(LANES * part + 32 * ((slot + place[1]) & 3), 32), 32)
            gh[there, :] = fh[here, :]
            gl[there, :] = fl[here, :]
    for h in range(2):
        values = [
            tuple(lines[pl.ds(32 * r + 16 * h + part, 8, stride=2), :] for part in range(2)) for r in range(R)
        ]
        for k, (re, im) in enumerate(dft(values, -1)):
            a_re[k * 24 + 8 * h : k * 24 + 8 * h + 8, :] = re
            a_im[k * 24 + 8 * h : k * 24 + 8 * h + 8, :] = im

    def turn_c(c, h):
        rows = slice((c - 1) * R + 8 * h, (c - 1) * R + 8 * h + 8)
        if c <= 8:
            return cos_c[rows, :], sin_c[rows, :]
        rows = slice((c - 9) * R + 8 * h, (c - 9) * R + 8 * h + 8)
        return late_c[rows, :], late_s[rows, :]

    for h in range(4):
        values = []
        for c in range(C):
            re, im = a_re[pl.ds(8 * h * 24 + c, 8, stride=24), :], a_im[pl.ds(8 * h * 24 + c, 8, stride=24), :]
            if c > 8:
                (u, v), (w, z) = turn_c(c - 8, h), turn_c(8, h)
                rows = slice((c - 9) * R + 8 * h, (c - 9) * R + 8 * h + 8)
                late_c[rows, :], late_s[rows, :] = u * w - v * z, u * z + v * w
            if c:
                u, v = turn_c(c, h)
                re, im = re * u + im * v, im * u - re * v
            values.append((re, im))
        for k, (re, im) in enumerate(dft(values, -1)):
            rows = slice(h * LANES + 8 * k, h * LANES + 8 * k + 8)
            u, v = cos_r[8 * h : 8 * h + 8, :], sin_r[8 * h : 8 * h + 8, :]
            if k:
                c, d = cos_k[k : k + 1, :], sin_k[k : k + 1, :]
                u, v = u * c - v * d, u * d + v * c
            cos_i[rows, :], sin_i[rows, :] = u, v
            wide[rows, :LANES] = re * u + im * v
            wide[rows, LANES:] = im * u - re * v
    along_y, normal = column_factors(place)
    low_lanes = lane_of((8, LANES)) < 64
    for g in range(2):
        advanced = []
        for h in (2 * g, 2 * g + 1):
            rows = slice(h * LANES, (h + 1) * LANES)
            spectra = dot(halves(wide[rows, :]), (gh[...], gl[...]))
            linear = decay[rows, :] + along_y
            grown = jnp.exp(linear * (0.5 * TIME_STEP))
            growth, forcing = grown * (1.0 / (N * N)), (grown - 1.0) / linear * normal
            advanced.append(growth * spectra[:, :LANES] + forcing * spectra[:, 2 * LANES : 3 * LANES])
            advanced.append(growth * spectra[:, LANES : 2 * LANES] + forcing * spectra[:, 3 * LANES :])
        both = dot(halves(jnp.concatenate(advanced, axis=1)), (bh[...], bl[...]))
        values = []
        for k in range(C):
            rows = [slice(h * LANES + 8 * k, h * LANES + 8 * k + 8) for h in (2 * g, 2 * g + 1)]
            u, v = (jnp.where(low_lanes, t[rows[0], :], t[rows[1], :]) for t in (cos_i, sin_i))
            re, im = both[8 * k : 8 * k + 8, :LANES], both[8 * k : 8 * k + 8, LANES:]
            values.append((re * u - im * v, im * u + re * v))
        values = dft(values, 1)
        for c in range(1, C):
            first, second = turn_c(c, 2 * g), turn_c(c, 2 * g + 1)
            u, v = jnp.where(low_lanes, first[0], second[0]), jnp.where(low_lanes, first[1], second[1])
            re, im = values[c]
            values[c] = re * u - im * v, im * u + re * v
        for c in range(8):
            for part, kept in enumerate((a_re, a_im)):
                one, two = values[c][part], values[c + 8][part]
                kept[pl.ds(128 * g + c, 8, stride=8), :] = jnp.where(low_lanes, one, pltpu.roll(two, 64, 1))
                kept[pl.ds(128 * g + 64 + c, 8, stride=8), :] = jnp.where(low_lanes, pltpu.roll(one, 64, 1), two)
    on = 16 * (place[1] & 7)
    values = [(a_re[8 * k : 8 * k + 8, :], a_im[8 * k : 8 * k + 8, :]) for k in range(R)]
    for r, (re, im) in enumerate(dft(values, 1)):
        one = jnp.where(low_lanes, re, pltpu.roll(im, 64, 1))
        two = jnp.where(low_lanes, pltpu.roll(re, 64, 1), im)
        out[r * C : r * C + 8, :] = pltpu.roll(one, on, 1)
        out[r * C + 8 : r * C + 16, :] = pltpu.roll(two, on, 1)


def y_backward(pieces, cos_y, sin_y, high, low, out, spectrum, turned):
    lane = lane_of((R, LANES))
    for t in range(2):
        sources = [pieces[pl.ds(8 * t + j, R, stride=C), :] for j in range(8)]
        for b in range(8):
            block = by_block([sources[(k - b) % 8] for k in range(8)], 16, lane)
            block = pltpu.roll(block, LANES - 16 * b, 1) if b else block
            spectrum[b * R : (b + 1) * R, t * LANES : (t + 1) * LANES] = block
    flipped = spectrum[...].T
    turned[...] = dot(halves(flipped), (high[...], low[...]))
    parity = 1.0 - 2.0 * (lane_of((16, M)) & 1).astype(jnp.float32)
    values = []
    for k in range(C):
        re, im = turned[16 * k : 16 * (k + 1), :M], turned[16 * k : 16 * (k + 1), M:]
        if k == 0:
            re, im = re - flipped[:16, 0:1] + flipped[:16, 128:129] * parity, None
        else:
            u, v = cos_y[k : k + 1, :], sin_y[k : k + 1, :]
            re, im = re * u - im * v, im * u + re * v
        values.append((re, im))
    substrate_row = lax.broadcasted_iota(jnp.int32, (16, M), 0) < I
    constant = math.expm1(-0.5 * FEED_RATE * TIME_STEP) / -FEED_RATE * FEED_RATE
    shift = jnp.where(substrate_row, constant, 0.0)
    for c, (re, _) in enumerate(dft(values, 1)):
        out[c] = re + shift


def tables():
    f32 = np.float32
    angle = 2 * np.pi / N * (np.arange(C)[:, None] * np.arange(M)[None, :])
    cos_y, sin_y = np.cos(angle), np.sin(angle)
    turn_m = 2 * np.pi / M * (np.arange(M)[:, None] * np.arange(128)[None, :] % M)
    c, s = np.cos(turn_m), np.sin(turn_m)
    y_matrix = np.block([[c, -s], [s, c]])
    y_inverse = 2 * np.block([[c.T, s.T], [-s.T, c.T]])
    ones = np.ones((1, LANES))
    outer = np.arange(1, 9)[:, None] * np.arange(R)[None, :]
    angle = 2 * np.pi / D * outer.reshape(-1, 1) * ones
    cos_c, sin_c = np.cos(angle), np.sin(angle)
    lane_i = (np.arange(LANES) % I)[None, :]
    angle = 2 * np.pi / N * (np.arange(R)[:, None] * lane_i)
    cos_r, sin_r = np.cos(angle), np.sin(angle)
    angle = 2 * np.pi / 128 * (np.arange(C)[:, None] * lane_i % 128)
    cos_k, sin_k = np.cos(angle), np.sin(angle)
    angle = 2 * np.pi / I * (np.arange(I)[:, None] * np.arange(I)[None, :] % I)
    c, s = np.cos(angle), np.sin(angle)
    forward = np.zeros((2, LANES, 2, 2, LANES))
    backward = np.zeros((2, 2, LANES, 2, LANES))
    for slot in range(5):
        for field in range(2):
            here = slice(16 * slot + I * field, 16 * slot + I * field + I)
            for g in range(2):
                there = slice(64 * g + 16 * (slot % 4) + I * field, 64 * g + 16 * (slot % 4) + I * field + I)
                turn_i = ((c, -s), (s, c)) if slot < 4 else ((-s, -c), (c, -s))
                for part in range(2):
                    backward[g, 0, here, part, there] += turn_i[part][0]
                    backward[g, 1, here, part, there] += turn_i[part][1]
            for kind, taken in enumerate((field, 2)):
                start = 32 * slot + I * taken if slot < 4 else 32 * taken + 3 * I
                there = slice(start, start + I)
                forward[0, there, kind, 0, here], forward[1, there, kind, 0, here] = c, s
                forward[0, there, kind, 1, here], forward[1, there, kind, 1, here] = -s, c
    forward = forward.reshape(2 * LANES, 4 * LANES)
    backward = backward.reshape(4 * LANES, 2 * LANES)
    lane = np.arange(LANES)[None, :]
    row = np.arange(D)[:, None]
    p = 8 * (row // LANES) + row % 8 + R * (row % LANES // 8) + D * (lane % I)
    angular = 2 * np.pi * np.where(2 * p < N, p, p - N)
    decay = -np.where(lane // I % 2 == 0, SUBSTRATE_DIFFUSION, ACTIVATOR_DIFFUSION) * angular**2

    def parts(matrix):
        high = matrix.astype(np.float32).astype(jnp.bfloat16)
        return high, (matrix - high.astype(np.float64)).astype(jnp.bfloat16)

    along_y = [a.astype(f32) for a in (cos_y, sin_y)]
    along_x = [a.astype(f32) for a in (cos_c, sin_c, cos_r, sin_r, cos_k, sin_k, decay)]
    return (
        (*along_y, *parts(y_matrix)),
        (*along_x, *parts(forward), *parts(backward)),
        (*along_y, *parts(y_inverse)),
    )


def column_factors(place):
    lane = lane_of((1, LANES))
    slot = lane >> 4
    q = jnp.where(slot == 4, N // 2, place[1] + C * (R * (slot & 3) + place[0]))
    signed = jnp.where(2 * q < N, q, q - N).astype(jnp.float32)
    angular = 2.0 * math.pi * signed
    substrate = (lane & I) == 0
    diffusion = jnp.where(substrate, SUBSTRATE_DIFFUSION, ACTIVATOR_DIFFUSION)
    decay = jnp.where(substrate, FEED_RATE, FEED_RATE + KILL_RATE)
    normalize = 1.0 / (N * N)
    return -diffusion * (angular * angular) - decay, jnp.where(substrate, -normalize, normalize)


def call(body, out_shape, scratch, *operands):
    return pl.pallas_call(
        body,
        out_shape=jax.ShapeDtypeStruct(out_shape, jnp.float32),
        in_specs=[pl.BlockSpec(memory_space=pltpu.VMEM) for _ in operands],
        out_specs=pl.BlockSpec(memory_space=pltpu.VMEM),
        scratch_shapes=[pltpu.VMEM(shape[:2], *shape[2:] or (jnp.float32,)) for shape in scratch],
        compiler_params=pltpu.CompilerParams(vmem_limit_bytes=48 * 1024 * 1024),
    )(*operands)


def on_device(substrate, activator):
    along_y, along_x, back_y = tables()
    fields = jnp.concatenate([substrate.reshape(C, I, M), activator.reshape(C, I, M)], axis=1)
    fields = lax.all_to_all(fields, "col", 0, 0, tiled=True)
    pieces = call(y_forward, (2 * D, LANES), [(D, 2 * M)], fields, *along_y)
    lines = lax.all_to_all(pieces.reshape(D, 2, LANES), ALL, 0, 0, tiled=True).reshape(2 * D, LANES)
    scratch = [(24 * R, LANES)] * 2 + [(D, LANES)] * 2 + [(D, 2 * LANES)]
    scratch += [(2 * LANES, 4 * LANES, jnp.bfloat16)] * 2 + [(7 * R, LANES)] * 2
    pieces = call(x_section, (D, LANES), scratch, lines, *along_x)
    pieces = lax.all_to_all(pieces.reshape(D, 1, LANES), ALL, 0, 0, tiled=True).reshape(D, LANES)
    fields = call(y_backward, (C, 2 * I, M), [(M, M), (M, 2 * M)], pieces, *back_y)
    fields = lax.all_to_all(fields, "col", 0, 0, tiled=True)
    return (fields[:, :I].reshape(C * I, M), fields[:, I:].reshape(C * I, M))


def solution(mesh):
    split = Mesh(
        mesh.devices.reshape(8, 2, 2, mesh.shape["col"]), ("row_0", "row_1", "row_2", "col")
    )
    placed = (P(ROW, "col"), P(ROW, "col"))
    return jax.shard_map(on_device, mesh=split, in_specs=placed, out_specs=placed, check_vma=False)
```

```python
import math

import jax
import jax.numpy as jnp
import numpy as np
from jax import lax
from jax.experimental import pallas as pl
from jax.experimental.pallas import tpu as pltpu
from jax.sharding import Mesh
from jax.sharding import PartitionSpec as P

ROW = ("row_0", "row_1", "row_2")
ROW_BY_CORE = ("row_2", "row_0", "row_1")
ALL = (*ROW_BY_CORE, "col")

FEED_RATE = 0.037
KILL_RATE = 0.06
TIME_STEP = 8.0
SUBSTRATE_DIFFUSION = 4e-07
ACTIVATOR_DIFFUSION = 2e-07

N = 4096
R = 32
C = 16
I = 8
M = 256
D = R * C
LANES = 128


def add(a, b):
    return b if a is None else a if b is None else a + b


def sub(a, b):
    return (None if b is None else -b) if a is None else a if b is None else a - b


def scale(a, c):
    if a is None or c == 0.0:
        return None
    return a if c == 1.0 else -a if c == -1.0 else a * c


def turn(z, k, n, sign):
    c, s = unit(k, n, sign)
    return sub(scale(z[0], c), scale(z[1], s)), add(scale(z[0], s), scale(z[1], c))


def unit(k, n, sign):
    quarter, rest = divmod(4 * (k % n), n)
    if rest == 0:
        c, s = ((1.0, 0.0), (0.0, 1.0), (-1.0, 0.0), (0.0, -1.0))[quarter]
    else:
        c, s = math.cos(2 * math.pi * k / n), math.sin(2 * math.pi * k / n)
    return c, sign * s


def dft(values, sign):
    n = len(values)
    if n == 1:
        return values
    even, odd = dft(values[0::2], sign), dft(values[1::2], sign)
    odd = [turn(z, k, n, sign) for k, z in enumerate(odd)]
    pairs = list(zip(even, odd))
    return [(add(e[0], o[0]), add(e[1], o[1])) for e, o in pairs] + [
        (sub(e[0], o[0]), sub(e[1], o[1])) for e, o in pairs
    ]


def real_dft(values):
    n = len(values)
    if n == 2:
        return [(add(*values), None), (sub(*values), None)]
    even, odd = real_dft(values[0::2]), real_dft(values[1::2])
    odd = [turn(z, k, n, -1) for k, z in enumerate(odd)]
    low = [(add(e[0], o[0]), add(e[1], o[1])) for e, o in zip(even, odd)]
    high = [(sub(e[0], o[0]), sub(o[1], e[1])) for e, o in zip(even, odd)]
    return low + high[: n // 4][::-1]


def halves(a):
    high = a.astype(jnp.bfloat16)
    return high, (a - high.astype(jnp.float32)).astype(jnp.bfloat16)


def dot(a, b, dims=((1,), (0,))):
    def product(u, v):
        return lax.dot_general(u, v, (dims, ((), ())), preferred_element_type=jnp.float32)

    return product(a[0], b[0]) + (product(a[1], b[0]) + product(a[0], b[1]))


def lane_of(shape):
    return lax.broadcasted_iota(jnp.int32, shape, len(shape) - 1)


def by_block(sources, width, lane):
    piece = sources[0]
    for k, source in enumerate(sources[1:], 1):
        piece = jnp.where(lane >= width * k, source, piece)
    return piece


def y_forward(fields, cos_y, sin_y, high, low, out, turned):
    for f in range(3):
        lines = []
        for c in range(C):
            if f < 2:
                lines.append(fields[c, f * I : (f + 1) * I, :])
            else:
                a = fields[c, I:, :]
                lines.append(fields[c, :I, :] * a * a)
        half = real_dft(lines)
        for k in range(C):
            re, im = half[k] if k <= C // 2 else half[C - k]
            if im is not None and k > C // 2:
                im = -im
            if k:
                c, s = cos_y[k : k + 1, :], sin_y[k : k + 1, :]
                if im is None:
                    re, im = re * c, -re * s
                else:
                    re, im = re * c + im * s, im * c - re * s
            else:
                im = jnp.zeros_like(re)
            row = k * 32 + f * I
            turned[row : row + I, :M] = re
            turned[row : row + I, M:] = im
    for k in range(C):
        row = k * 32 + 3 * I
        turned[row : row + I, :] = jnp.zeros((I, 2 * M), jnp.float32)
    parity = 1.0 - 2.0 * (lane_of((I, M)) & 1).astype(jnp.float32)
    place = lane_of((I, LANES))
    last = jnp.zeros((I, LANES), jnp.float32)
    for f in range(3):
        total = jnp.sum(turned[f * I : (f + 1) * I, :M] * parity, axis=1, keepdims=True)
        last = jnp.where(place == 32 * f, total, last)
    lane = lane_of((R, LANES))
    for t in range(4):
        spectra = dot(halves(turned[t * LANES : (t + 1) * LANES, :]), (high[...], low[...]))
        for part in range(2):
            half = spectra[:, part * LANES : (part + 1) * LANES]
            if t == 0 and part == 0:
                half = jnp.concatenate([half[: 3 * I], last, half[4 * I :]], axis=0)
            half = half.T
            blocks = [half[32 * s : 32 * (s + 1), :] for s in range(4)]
            blocks = [blocks[0]] + [pltpu.roll(blocks[s], 32 * s, 1) for s in range(1, 4)]
            for j in range(4):
                piece = by_block([blocks[(k - j) % 4] for k in range(4)], 32, lane)
                out[pl.ds((4 * t + j) * 2 + part, R, stride=2 * C), :] = piece


def sent(r):
    return r % 2 * (R // 2) + r // 2


def x_section(
    lines, cos_c, sin_c, cos_r, sin_r, cos_k, sin_k, decay, fh, fl, bh, bl, out, a_re, a_im, cos_i, sin_i, wide, gh, gl, late_c, late_s
):
    place = lax.axis_index(ROW_BY_CORE), lax.axis_index("col")
    for part in range(2):
        for slot in range(4):
            here = slice(LANES * part + 32 * slot, LANES * part + 32 * (slot + 1))
            there = pl.ds(pl.multiple_of(LANES * part + 32 * ((slot + place[1]) & 3), 32), 32)
            gh[there, :] = fh[here, :]
            gl[there, :] = fl[here, :]
    for h in range(2):
        values = [
            tuple(lines[pl.ds(32 * sent(r) + 16 * h + part, 8, stride=2), :] for part in range(2))
            for r in range(R)
        ]
        for k, (re, im) in enumerate(dft(values, -1)):
            a_re[k * 24 + 8 * h : k * 24 + 8 * h + 8, :] = re
            a_im[k * 24 + 8 * h : k * 24 + 8 * h + 8, :] = im

    def turn_c(c, h):
        rows = slice((c - 1) * R + 8 * h, (c - 1) * R + 8 * h + 8)
        if c <= 8:
            return cos_c[rows, :], sin_c[rows, :]
        rows = slice((c - 9) * R + 8 * h, (c - 9) * R + 8 * h + 8)
        return late_c[rows, :], late_s[rows, :]

    for h in range(4):
        values = []
        for c in range(C):
            re, im = a_re[pl.ds(8 * h * 24 + c, 8, stride=24), :], a_im[pl.ds(8 * h * 24 + c, 8, stride=24), :]
            if c > 8:
                (u, v), (w, z) = turn_c(c - 8, h), turn_c(8, h)
                rows = slice((c - 9) * R + 8 * h, (c - 9) * R + 8 * h + 8)
                late_c[rows, :], late_s[rows, :] = u * w - v * z, u * z + v * w
            if c:
                u, v = turn_c(c, h)
                re, im = re * u + im * v, im * u - re * v
            values.append((re, im))
        for k, (re, im) in enumerate(dft(values, -1)):
            rows = slice(h * LANES + 8 * k, h * LANES + 8 * k + 8)
            u, v = cos_r[8 * h : 8 * h + 8, :], sin_r[8 * h : 8 * h + 8, :]
            if k:
                c, d = cos_k[k : k + 1, :], sin_k[k : k + 1, :]
                u, v = u * c - v * d, u * d + v * c
            cos_i[rows, :], sin_i[rows, :] = u, v
            wide[rows, :LANES] = re * u + im * v
            wide[rows, LANES:] = im * u - re * v
    along_y, normal = column_factors(place)
    low_lanes = lane_of((8, LANES)) < 64
    for g in range(2):
        advanced = []
        for h in (2 * g, 2 * g + 1):
            rows = slice(h * LANES, (h + 1) * LANES)
            spectra = dot(halves(wide[rows, :]), (gh[...], gl[...]))
            linear = decay[rows, :] + along_y
            grown = jnp.exp(linear * (0.5 * TIME_STEP))
            growth, forcing = grown * (1.0 / (N * N)), (grown - 1.0) / linear * normal
            advanced.append(growth * spectra[:, :LANES] + forcing * spectra[:, 2 * LANES : 3 * LANES])
            advanced.append(growth * spectra[:, LANES : 2 * LANES] + forcing * spectra[:, 3 * LANES :])
        both = dot(halves(jnp.concatenate(advanced, axis=1)), (bh[...], bl[...]))
        values = []
        for k in range(C):
            rows = [slice(h * LANES + 8 * k, h * LANES + 8 * k + 8) for h in (2 * g, 2 * g + 1)]
            u, v = (jnp.where(low_lanes, t[rows[0], :], t[rows[1], :]) for t in (cos_i, sin_i))
            re, im = both[8 * k : 8 * k + 8, :LANES], both[8 * k : 8 * k + 8, LANES:]
            values.append((re * u - im * v, im * u + re * v))
        values = dft(values, 1)
        for c in range(1, C):
            first, second = turn_c(c, 2 * g), turn_c(c, 2 * g + 1)
            u, v = jnp.where(low_lanes, first[0], second[0]), jnp.where(low_lanes, first[1], second[1])
            re, im = values[c]
            values[c] = re * u - im * v, im * u + re * v
        for c in range(8):
            for part, kept in enumerate((a_re, a_im)):
                one, two = values[c][part], values[c + 8][part]
                kept[pl.ds(128 * g + c, 8, stride=8), :] = jnp.where(low_lanes, one, pltpu.roll(two, 64, 1))
                kept[pl.ds(128 * g + 64 + c, 8, stride=8), :] = jnp.where(low_lanes, pltpu.roll(one, 64, 1), two)
    on = 16 * (place[1] & 7)
    values = [(a_re[8 * k : 8 * k + 8, :], a_im[8 * k : 8 * k + 8, :]) for k in range(R)]
    for r, (re, im) in enumerate(dft(values, 1)):
        one = jnp.where(low_lanes, re, pltpu.roll(im, 64, 1))
        two = jnp.where(low_lanes, pltpu.roll(re, 64, 1), im)
        row = C * sent(r)
        out[row : row + 8, :] = pltpu.roll(one, on, 1)
        out[row + 8 : row + 16, :] = pltpu.roll(two, on, 1)


def y_backward(pieces, cos_y, sin_y, high, low, out, spectrum, turned):
    lane = lane_of((R, LANES))
    for t in range(2):
        sources = [pieces[pl.ds(8 * t + j, R, stride=C), :] for j in range(8)]
        for b in range(8):
            block = by_block([sources[(k - b) % 8] for k in range(8)], 16, lane)
            block = pltpu.roll(block, LANES - 16 * b, 1) if b else block
            spectrum[b * R : (b + 1) * R, t * LANES : (t + 1) * LANES] = block
    flipped = spectrum[...].T
    turned[...] = dot(halves(flipped), (high[...], low[...]))
    parity = 1.0 - 2.0 * (lane_of((16, M)) & 1).astype(jnp.float32)
    values = []
    for k in range(C):
        re, im = turned[16 * k : 16 * (k + 1), :M], turned[16 * k : 16 * (k + 1), M:]
        if k == 0:
            re, im = re - flipped[:16, 0:1] + flipped[:16, 128:129] * parity, None
        else:
            u, v = cos_y[k : k + 1, :], sin_y[k : k + 1, :]
            re, im = re * u - im * v, im * u + re * v
        values.append((re, im))
    substrate_row = lax.broadcasted_iota(jnp.int32, (16, M), 0) < I
    constant = math.expm1(-0.5 * FEED_RATE * TIME_STEP) / -FEED_RATE * FEED_RATE
    shift = jnp.where(substrate_row, constant, 0.0)
    for c, (re, _) in enumerate(dft(values, 1)):
        out[c] = re + shift


def tables():
    f32 = np.float32
    angle = 2 * np.pi / N * (np.arange(C)[:, None] * np.arange(M)[None, :])
    cos_y, sin_y = np.cos(angle), np.sin(angle)
    turn_m = 2 * np.pi / M * (np.arange(M)[:, None] * np.arange(128)[None, :] % M)
    c, s = np.cos(turn_m), np.sin(turn_m)
    y_matrix = np.block([[c, -s], [s, c]])
    y_inverse = 2 * np.block([[c.T, s.T], [-s.T, c.T]])
    ones = np.ones((1, LANES))
    outer = np.arange(1, 9)[:, None] * np.arange(R)[None, :]
    angle = 2 * np.pi / D * outer.reshape(-1, 1) * ones
    cos_c, sin_c = np.cos(angle), np.sin(angle)
    lane_i = (np.arange(LANES) % I)[None, :]
    angle = 2 * np.pi / N * (np.arange(R)[:, None] * lane_i)
    cos_r, sin_r = np.cos(angle), np.sin(angle)
    angle = 2 * np.pi / 128 * (np.arange(C)[:, None] * lane_i % 128)
    cos_k, sin_k = np.cos(angle), np.sin(angle)
    angle = 2 * np.pi / I * (np.arange(I)[:, None] * np.arange(I)[None, :] % I)
    c, s = np.cos(angle), np.sin(angle)
    forward = np.zeros((2, LANES, 2, 2, LANES))
    backward = np.zeros((2, 2, LANES, 2, LANES))
    for slot in range(5):
        for field in range(2):
            here = slice(16 * slot + I * field, 16 * slot + I * field + I)
            for g in range(2):
                there = slice(64 * g + 16 * (slot % 4) + I * field, 64 * g + 16 * (slot % 4) + I * field + I)
                turn_i = ((c, -s), (s, c)) if slot < 4 else ((-s, -c), (c, -s))
                for part in range(2):
                    backward[g, 0, here, part, there] += turn_i[part][0]
                    backward[g, 1, here, part, there] += turn_i[part][1]
            for kind, taken in enumerate((field, 2)):
                start = 32 * slot + I * taken if slot < 4 else 32 * taken + 3 * I
                there = slice(start, start + I)
                forward[0, there, kind, 0, here], forward[1, there, kind, 0, here] = c, s
                forward[0, there, kind, 1, here], forward[1, there, kind, 1, here] = -s, c
    forward = forward.reshape(2 * LANES, 4 * LANES)
    backward = backward.reshape(4 * LANES, 2 * LANES)
    lane = np.arange(LANES)[None, :]
    row = np.arange(D)[:, None]
    p = 8 * (row // LANES) + row % 8 + R * (row % LANES // 8) + D * (lane % I)
    angular = 2 * np.pi * np.where(2 * p < N, p, p - N)
    decay = -np.where(lane // I % 2 == 0, SUBSTRATE_DIFFUSION, ACTIVATOR_DIFFUSION) * angular**2

    def parts(matrix):
        high = matrix.astype(np.float32).astype(jnp.bfloat16)
        return high, (matrix - high.astype(np.float64)).astype(jnp.bfloat16)

    along_y = [a.astype(f32) for a in (cos_y, sin_y)]
    along_x = [a.astype(f32) for a in (cos_c, sin_c, cos_r, sin_r, cos_k, sin_k, decay)]
    return (
        (*along_y, *parts(y_matrix)),
        (*along_x, *parts(forward), *parts(backward)),
        (*along_y, *parts(y_inverse)),
    )


def column_factors(place):
    lane = lane_of((1, LANES))
    slot = lane >> 4
    q = jnp.where(slot == 4, N // 2, place[1] + C * (R * (slot & 3) + place[0]))
    signed = jnp.where(2 * q < N, q, q - N).astype(jnp.float32)
    angular = 2.0 * math.pi * signed
    substrate = (lane & I) == 0
    diffusion = jnp.where(substrate, SUBSTRATE_DIFFUSION, ACTIVATOR_DIFFUSION)
    decay = jnp.where(substrate, FEED_RATE, FEED_RATE + KILL_RATE)
    normalize = 1.0 / (N * N)
    return -diffusion * (angular * angular) - decay, jnp.where(substrate, -normalize, normalize)


def call(body, out_shape, scratch, *operands):
    return pl.pallas_call(
        body,
        out_shape=jax.ShapeDtypeStruct(out_shape, jnp.float32),
        in_specs=[pl.BlockSpec(memory_space=pltpu.VMEM) for _ in operands],
        out_specs=pl.BlockSpec(memory_space=pltpu.VMEM),
        scratch_shapes=[pltpu.VMEM(shape[:2], *shape[2:] or (jnp.float32,)) for shape in scratch],
        compiler_params=pltpu.CompilerParams(vmem_limit_bytes=48 * 1024 * 1024),
    )(*operands)


def on_device(substrate, activator):
    along_y, along_x, back_y = tables()
    fields = jnp.concatenate([substrate.reshape(C, I, M), activator.reshape(C, I, M)], axis=1)
    fields = lax.all_to_all(fields, "col", 0, 0, tiled=True)
    pieces = call(y_forward, (2 * D, LANES), [(D, 2 * M)], fields, *along_y)
    lines = lax.all_to_all(pieces.reshape(D, 2, LANES), ALL, 0, 0, tiled=True).reshape(2 * D, LANES)
    scratch = [(24 * R, LANES)] * 2 + [(D, LANES)] * 2 + [(D, 2 * LANES)]
    scratch += [(2 * LANES, 4 * LANES, jnp.bfloat16)] * 2 + [(7 * R, LANES)] * 2
    pieces = call(x_section, (D, LANES), scratch, lines, *along_x)
    pieces = lax.all_to_all(pieces.reshape(D, 1, LANES), ALL, 0, 0, tiled=True).reshape(D, LANES)
    fields = call(y_backward, (C, 2 * I, M), [(M, M), (M, 2 * M)], pieces, *back_y)
    fields = lax.all_to_all(fields, "col", 0, 0, tiled=True)
    return (fields[:, :I].reshape(C * I, M), fields[:, I:].reshape(C * I, M))


def solution(mesh):
    split = Mesh(
        mesh.devices.reshape(8, 2, 2, mesh.shape["col"]), ("row_0", "row_1", "row_2", "col")
    )
    placed = (P(ROW, "col"), P(ROW, "col"))
    return jax.shard_map(on_device, mesh=split, in_specs=placed, out_specs=placed, check_vma=False)
```

```python
import math

import jax
import jax.numpy as jnp
import numpy as np
from jax import lax
from jax.experimental import pallas as pl
from jax.experimental.pallas import tpu as pltpu
from jax.sharding import Mesh
from jax.sharding import PartitionSpec as P

ROW = ("row_0", "row_1", "row_2")
ALL = ("row_0", "row_1", "row_2", "col")

FEED_RATE = 0.037
KILL_RATE = 0.06
TIME_STEP = 8.0
SUBSTRATE_DIFFUSION = 4e-07
ACTIVATOR_DIFFUSION = 2e-07

N = 4096
R = 32
C = 16
I = 8
M = 256
D = R * C
LANES = 128


def add(a, b):
    return b if a is None else a if b is None else a + b


def sub(a, b):
    return (None if b is None else -b) if a is None else a if b is None else a - b


def scale(a, c):
    if a is None or c == 0.0:
        return None
    return a if c == 1.0 else -a if c == -1.0 else a * c


def turn(z, k, n, sign):
    c, s = unit(k, n, sign)
    return sub(scale(z[0], c), scale(z[1], s)), add(scale(z[0], s), scale(z[1], c))


def unit(k, n, sign):
    quarter, rest = divmod(4 * (k % n), n)
    if rest == 0:
        c, s = ((1.0, 0.0), (0.0, 1.0), (-1.0, 0.0), (0.0, -1.0))[quarter]
    else:
        c, s = math.cos(2 * math.pi * k / n), math.sin(2 * math.pi * k / n)
    return c, sign * s


def dft(values, sign):
    n = len(values)
    if n == 1:
        return values
    even, odd = dft(values[0::2], sign), dft(values[1::2], sign)
    odd = [turn(z, k, n, sign) for k, z in enumerate(odd)]
    pairs = list(zip(even, odd))
    return [(add(e[0], o[0]), add(e[1], o[1])) for e, o in pairs] + [
        (sub(e[0], o[0]), sub(e[1], o[1])) for e, o in pairs
    ]


def real_dft(values):
    n = len(values)
    if n == 2:
        return [(add(*values), None), (sub(*values), None)]
    even, odd = real_dft(values[0::2]), real_dft(values[1::2])
    odd = [turn(z, k, n, -1) for k, z in enumerate(odd)]
    low = [(add(e[0], o[0]), add(e[1], o[1])) for e, o in zip(even, odd)]
    high = [(sub(e[0], o[0]), sub(o[1], e[1])) for e, o in zip(even, odd)]
    return low + high[: n // 4][::-1]


def halves(a):
    high = a.astype(jnp.bfloat16)
    return high, (a - high.astype(jnp.float32)).astype(jnp.bfloat16)


def dot(a, b, dims=((1,), (0,))):
    def product(u, v):
        return lax.dot_general(u, v, (dims, ((), ())), preferred_element_type=jnp.float32)

    return product(a[0], b[0]) + (product(a[1], b[0]) + product(a[0], b[1]))


def lane_of(shape):
    return lax.broadcasted_iota(jnp.int32, shape, len(shape) - 1)


def by_block(sources, width, lane):
    piece = sources[0]
    for k, source in enumerate(sources[1:], 1):
        piece = jnp.where(lane >= width * k, source, piece)
    return piece


def y_forward(fields, cos_y, sin_y, high, low, out, turned):
    for f in range(3):
        lines = []
        for c in range(C):
            if f < 2:
                lines.append(fields[c, f * I : (f + 1) * I, :])
            else:
                a = fields[c, I:, :]
                lines.append(fields[c, :I, :] * a * a)
        half = real_dft(lines)
        for k in range(C):
            re, im = half[k] if k <= C // 2 else half[C - k]
            if im is not None and k > C // 2:
                im = -im
            if k:
                c, s = cos_y[k : k + 1, :], sin_y[k : k + 1, :]
                if im is None:
                    re, im = re * c, -re * s
                else:
                    re, im = re * c + im * s, im * c - re * s
            else:
                im = jnp.zeros_like(re)
            row = k * 32 + f * I
            turned[row : row + I, :M] = re
            turned[row : row + I, M:] = im
    for k in range(C):
        row = k * 32 + 3 * I
        turned[row : row + I, :] = jnp.zeros((I, 2 * M), jnp.float32)
    parity = 1.0 - 2.0 * (lane_of((I, M)) & 1).astype(jnp.float32)
    place = lane_of((I, LANES))
    last = jnp.zeros((I, LANES), jnp.float32)
    for f in range(3):
        total = jnp.sum(turned[f * I : (f + 1) * I, :M] * parity, axis=1, keepdims=True)
        last = jnp.where(place == 32 * f, total, last)
    lane = lane_of((R, LANES))
    for t in range(4):
        spectra = dot(halves(turned[t * LANES : (t + 1) * LANES, :]), (high[...], low[...]))
        for part in range(2):
            half = spectra[:, part * LANES : (part + 1) * LANES]
            if t == 0 and part == 0:
                half = jnp.concatenate([half[: 3 * I], last, half[4 * I :]], axis=0)
            half = half.T
            blocks = [half[32 * s : 32 * (s + 1), :] for s in range(4)]
            blocks = [blocks[0]] + [pltpu.roll(blocks[s], 32 * s, 1) for s in range(1, 4)]
            for j in range(4):
                piece = by_block([blocks[(k - j) % 4] for k in range(4)], 32, lane)
                out[pl.ds((4 * t + j) * 2 + part, R, stride=2 * C), :] = piece


def x_section(
    lines, cos_c, sin_c, cos_r, sin_r, cos_k, sin_k, decay, fh, fl, bh, bl, out, a_re, a_im, cos_i, sin_i, wide, gh, gl, late_c, late_s
):
    place = lax.axis_index(ROW), lax.axis_index("col")
    for part in range(2):
        for slot in range(4):
            here = slice(LANES * part + 32 * slot, LANES * part + 32 * (slot + 1))
            there = pl.ds(pl.multiple_of(LANES * part + 32 * ((slot + place[1]) & 3), 32), 32)
            gh[there, :] = fh[here, :]
            gl[there, :] = fl[here, :]
    for h in range(2):
        values = [
            tuple(lines[pl.ds(32 * r + 16 * h + part, 8, stride=2), :] for part in range(2)) for r in range(R)
        ]
        for k, (re, im) in enumerate(dft(values, -1)):
            a_re[k * 24 + 8 * h : k * 24 + 8 * h + 8, :] = re
            a_im[k * 24 + 8 * h : k * 24 + 8 * h + 8, :] = im

    def turn_c(c, h):
        rows = slice((c - 1) * R + 8 * h, (c - 1) * R + 8 * h + 8)
        if c <= 8:
            return cos_c[rows, :], sin_c[rows, :]
        rows = slice((c - 9) * R + 8 * h, (c - 9) * R + 8 * h + 8)
        return late_c[rows, :], late_s[rows, :]

    for h in range(4):
        values = []
        for c in range(C):
            re, im = a_re[pl.ds(8 * h * 24 + c, 8, stride=24), :], a_im[pl.ds(8 * h * 24 + c, 8, stride=24), :]
            if c > 8:
                (u, v), (w, z) = turn_c(c - 8, h), turn_c(8, h)
                rows = slice((c - 9) * R + 8 * h, (c - 9) * R + 8 * h + 8)
                late_c[rows, :], late_s[rows, :] = u * w - v * z, u * z + v * w
            if c:
                u, v = turn_c(c, h)
                re, im = re * u + im * v, im * u - re * v
            values.append((re, im))
        for k, (re, im) in enumerate(dft(values, -1)):
            rows = slice(h * LANES + 8 * k, h * LANES + 8 * k + 8)
            u, v = cos_r[8 * h : 8 * h + 8, :], sin_r[8 * h : 8 * h + 8, :]
            if k:
                c, d = cos_k[k : k + 1, :], sin_k[k : k + 1, :]
                u, v = u * c - v * d, u * d + v * c
            cos_i[rows, :], sin_i[rows, :] = u, v
            wide[rows, :LANES] = re * u + im * v
            wide[rows, LANES:] = im * u - re * v
    along_y = column_factors(place)
    low_lanes = lane_of((8, LANES)) < 64
    for g in range(2):
        advanced = []
        for h in (2 * g, 2 * g + 1):
            rows = slice(h * LANES, (h + 1) * LANES)
            spectra = dot(halves(wide[rows, :]), (gh[...], gl[...]))
            linear = decay[rows, :] + along_y
            grown = jnp.exp(linear * (0.5 * TIME_STEP))
            growth, forcing = grown, (grown - 1.0) / linear
            advanced.append(growth * spectra[:, :LANES] + forcing * spectra[:, 2 * LANES : 3 * LANES])
            advanced.append(growth * spectra[:, LANES : 2 * LANES] + forcing * spectra[:, 3 * LANES :])
        both = dot(halves(jnp.concatenate(advanced, axis=1)), (bh[...], bl[...]))
        values = []
        for k in range(C):
            rows = [slice(h * LANES + 8 * k, h * LANES + 8 * k + 8) for h in (2 * g, 2 * g + 1)]
            u, v = (jnp.where(low_lanes, t[rows[0], :], t[rows[1], :]) for t in (cos_i, sin_i))
            re, im = both[8 * k : 8 * k + 8, :LANES], both[8 * k : 8 * k + 8, LANES:]
            values.append((re * u - im * v, im * u + re * v))
        values = dft(values, 1)
        for c in range(1, C):
            first, second = turn_c(c, 2 * g), turn_c(c, 2 * g + 1)
            u, v = jnp.where(low_lanes, first[0], second[0]), jnp.where(low_lanes, first[1], second[1])
            re, im = values[c]
            values[c] = re * u - im * v, im * u + re * v
        for c in range(8):
            for part, kept in enumerate((a_re, a_im)):
                one, two = values[c][part], values[c + 8][part]
                kept[pl.ds(128 * g + c, 8, stride=8), :] = jnp.where(low_lanes, one, pltpu.roll(two, 64, 1))
                kept[pl.ds(128 * g + 64 + c, 8, stride=8), :] = jnp.where(low_lanes, pltpu.roll(one, 64, 1), two)
    on = 16 * (place[1] & 7)
    values = [(a_re[8 * k : 8 * k + 8, :], a_im[8 * k : 8 * k + 8, :]) for k in range(R)]
    for r, (re, im) in enumerate(dft(values, 1)):
        one = jnp.where(low_lanes, re, pltpu.roll(im, 64, 1))
        two = jnp.where(low_lanes, pltpu.roll(re, 64, 1), im)
        out[r * C : r * C + 8, :] = pltpu.roll(one, on, 1)
        out[r * C + 8 : r * C + 16, :] = pltpu.roll(two, on, 1)


def y_backward(pieces, cos_y, sin_y, high, low, out, spectrum, turned):
    lane = lane_of((R, LANES))
    for t in range(2):
        sources = [pieces[pl.ds(8 * t + j, R, stride=C), :] for j in range(8)]
        for b in range(8):
            block = by_block([sources[(k - b) % 8] for k in range(8)], 16, lane)
            block = pltpu.roll(block, LANES - 16 * b, 1) if b else block
            spectrum[b * R : (b + 1) * R, t * LANES : (t + 1) * LANES] = block
    flipped = spectrum[...].T
    turned[...] = dot(halves(flipped), (high[...], low[...]))
    parity = 1.0 - 2.0 * (lane_of((16, M)) & 1).astype(jnp.float32)
    values = []
    for k in range(C):
        re, im = turned[16 * k : 16 * (k + 1), :M], turned[16 * k : 16 * (k + 1), M:]
        if k == 0:
            re, im = re - flipped[:16, 0:1] + flipped[:16, 128:129] * parity, None
        else:
            u, v = cos_y[k : k + 1, :], sin_y[k : k + 1, :]
            re, im = re * u - im * v, im * u + re * v
        values.append((re, im))
    substrate_row = lax.broadcasted_iota(jnp.int32, (16, M), 0) < I
    constant = math.expm1(-0.5 * FEED_RATE * TIME_STEP) / -FEED_RATE * FEED_RATE
    shift = jnp.where(substrate_row, constant, 0.0)
    for c, (re, _) in enumerate(dft(values, 1)):
        out[c] = re + shift


def tables():
    f32 = np.float32
    angle = 2 * np.pi / N * (np.arange(C)[:, None] * np.arange(M)[None, :])
    cos_y, sin_y = np.cos(angle), np.sin(angle)
    turn_m = 2 * np.pi / M * (np.arange(M)[:, None] * np.arange(128)[None, :] % M)
    c, s = np.cos(turn_m), np.sin(turn_m)
    y_matrix = np.block([[c, -s], [s, c]])
    y_inverse = 2 * np.block([[c.T, s.T], [-s.T, c.T]])
    ones = np.ones((1, LANES))
    outer = np.arange(1, 9)[:, None] * np.arange(R)[None, :]
    angle = 2 * np.pi / D * outer.reshape(-1, 1) * ones
    cos_c, sin_c = np.cos(angle), np.sin(angle)
    lane_i = (np.arange(LANES) % I)[None, :]
    angle = 2 * np.pi / N * (np.arange(R)[:, None] * lane_i)
    cos_r, sin_r = np.cos(angle), np.sin(angle)
    angle = 2 * np.pi / 128 * (np.arange(C)[:, None] * lane_i % 128)
    cos_k, sin_k = np.cos(angle), np.sin(angle)
    angle = 2 * np.pi / I * (np.arange(I)[:, None] * np.arange(I)[None, :] % I)
    c, s = np.cos(angle), np.sin(angle)
    forward = np.zeros((2, LANES, 2, 2, LANES))
    backward = np.zeros((2, 2, LANES, 2, LANES))
    for slot in range(5):
        for field in range(2):
            here = slice(16 * slot + I * field, 16 * slot + I * field + I)
            for g in range(2):
                there = slice(64 * g + 16 * (slot % 4) + I * field, 64 * g + 16 * (slot % 4) + I * field + I)
                turn_i = ((c, -s), (s, c)) if slot < 4 else ((-s, -c), (c, -s))
                for part in range(2):
                    backward[g, 0, here, part, there] += turn_i[part][0]
                    backward[g, 1, here, part, there] += turn_i[part][1]
            for kind, taken in enumerate((field, 2)):
                start = 32 * slot + I * taken if slot < 4 else 32 * taken + 3 * I
                there = slice(start, start + I)
                forward[0, there, kind, 0, here], forward[1, there, kind, 0, here] = c, s
                forward[0, there, kind, 1, here], forward[1, there, kind, 1, here] = -s, c
    for slot in range(5):
        forward[:, :, 1, :, 16 * slot : 16 * slot + I] *= -1
    forward = forward.reshape(2 * LANES, 4 * LANES)
    backward = backward.reshape(4 * LANES, 2 * LANES) / (N * N)
    lane = np.arange(LANES)[None, :]
    row = np.arange(D)[:, None]
    p = 8 * (row // LANES) + row % 8 + R * (row % LANES // 8) + D * (lane % I)
    angular = 2 * np.pi * np.where(2 * p < N, p, p - N)
    decay = -np.where(lane // I % 2 == 0, SUBSTRATE_DIFFUSION, ACTIVATOR_DIFFUSION) * angular**2

    def parts(matrix):
        high = matrix.astype(np.float32).astype(jnp.bfloat16)
        return high, (matrix - high.astype(np.float64)).astype(jnp.bfloat16)

    along_y = [a.astype(f32) for a in (cos_y, sin_y)]
    along_x = [a.astype(f32) for a in (cos_c, sin_c, cos_r, sin_r, cos_k, sin_k, decay)]
    return (
        (*along_y, *parts(y_matrix)),
        (*along_x, *parts(forward), *parts(backward)),
        (*along_y, *parts(y_inverse)),
    )


def column_factors(place):
    lane = lane_of((1, LANES))
    slot = lane >> 4
    q = jnp.where(slot == 4, N // 2, place[1] + C * (R * (slot & 3) + place[0]))
    signed = jnp.where(2 * q < N, q, q - N).astype(jnp.float32)
    angular = 2.0 * math.pi * signed
    substrate = (lane & I) == 0
    diffusion = jnp.where(substrate, SUBSTRATE_DIFFUSION, ACTIVATOR_DIFFUSION)
    decay = jnp.where(substrate, FEED_RATE, FEED_RATE + KILL_RATE)
    return -diffusion * (angular * angular) - decay


def call(body, out_shape, scratch, *operands):
    return pl.pallas_call(
        body,
        out_shape=jax.ShapeDtypeStruct(out_shape, jnp.float32),
        in_specs=[pl.BlockSpec(memory_space=pltpu.VMEM) for _ in operands],
        out_specs=pl.BlockSpec(memory_space=pltpu.VMEM),
        scratch_shapes=[pltpu.VMEM(shape[:2], *shape[2:] or (jnp.float32,)) for shape in scratch],
        compiler_params=pltpu.CompilerParams(vmem_limit_bytes=48 * 1024 * 1024),
    )(*operands)


def on_device(substrate, activator):
    along_y, along_x, back_y = tables()
    fields = jnp.concatenate([substrate.reshape(C, I, M), activator.reshape(C, I, M)], axis=1)
    fields = lax.all_to_all(fields, "col", 0, 0, tiled=True)
    pieces = call(y_forward, (2 * D, LANES), [(D, 2 * M)], fields, *along_y)
    lines = lax.all_to_all(pieces.reshape(D, 2, LANES), ALL, 0, 0, tiled=True).reshape(2 * D, LANES)
    scratch = [(24 * R, LANES)] * 2 + [(D, LANES)] * 2 + [(D, 2 * LANES)]
    scratch += [(2 * LANES, 4 * LANES, jnp.bfloat16)] * 2 + [(7 * R, LANES)] * 2
    pieces = call(x_section, (D, LANES), scratch, lines, *along_x)
    pieces = lax.all_to_all(pieces.reshape(D, 1, LANES), ALL, 0, 0, tiled=True).reshape(D, LANES)
    fields = call(y_backward, (C, 2 * I, M), [(M, M), (M, 2 * M)], pieces, *back_y)
    fields = lax.all_to_all(fields, "col", 0, 0, tiled=True)
    return (fields[:, :I].reshape(C * I, M), fields[:, I:].reshape(C * I, M))


def solution(mesh):
    split = Mesh(
        mesh.devices.reshape(8, 2, 2, mesh.shape["col"]), ("row_0", "row_1", "row_2", "col")
    )
    placed = (P(ROW, "col"), P(ROW, "col"))
    return jax.shard_map(on_device, mesh=split, in_specs=placed, out_specs=placed, check_vma=False)
```
